256 devices in a mesh: section: 8 (over y, core), mp: 32 (over x, z).
Axes of the slice: x: 4, y: 4, z: 8, core: 2. Of those that a mesh axis runs over, the one named last changes fastest.
Arguments:
- arriving: bfloat16 [8, 768, 8192], P('section', None, 'mp'), may hold values from -6 to 6
- norm_gain: bfloat16 [8, 8192], P('section'), may hold values from 0.099609375 to 1.8984375
- w_query: bfloat16 [8, 8192, 8192], P('section', 'mp'), may hold values from -26 to 26
- w_key: bfloat16 [8, 1024, 8192], P('section', 'mp'), may hold values from -1 to 1
- w_value: bfloat16 [8, 1024, 8192], P('section', 'mp'), may hold values from -0.25 to 0.25
- w_out: bfloat16 [8, 8192, 8192], P('section', 'mp'), may hold values from -0.0625 to 0.0625
Outputs:
- attended: bfloat16 [8, 768, 8192], P('section', 'mp')
- stream_next: bfloat16 [8, 768, 8192], P('section', 'mp')
The draws below stay inside these ranges and needn't reach their ends.
All inputs are finite; a program needn't handle non-finite values.
Results may differ from the reference program's by a relative error of at most 0.017.
Values may be sent and summed in bfloat16 or wider, within the bound.
A program may use at most 128 MiB of HBM per device.

```python
import math
import jax
import jax.numpy as jnp
from jax import lax

D = 8192
HD = 128
KV_HEADS = 8
HQ_DEV = 2
HEADS = 64
KVD = 1024
LENGTH = 768
SECTIONS = 8


def key_rows(key):
    fresh = jax.random.normal(jax.random.fold_in(key, 11), (SECTIONS, KVD, D), jnp.float32)
    return jnp.clip(fresh, -5.0, 5.0) / math.sqrt(D)


def draw_w_key(key, part):
    return key_rows(key).astype(jnp.bfloat16)


def draw_w_query(key, part):
    fresh = jax.random.normal(jax.random.fold_in(key, 23), (SECTIONS, HEADS * HD, D), jnp.float32)
    fresh = jnp.clip(fresh, -5.0, 5.0) / math.sqrt(D)
    return fresh.astype(jnp.bfloat16)


def shard_levels(own_key, shape, cuts, low, largest):
    level = 1.0
    for position, shards_of in cuts:
        draws = jax.random.uniform(jax.random.fold_in(jax.random.fold_in(own_key, 6), position), (shards_of,), jnp.float32, low / len(cuts), largest / len(cuts))
        level = level * jnp.repeat(jnp.exp(draws), shape[position] // shards_of).reshape((-1,) + (1,) * (len(shape) - 1 - position))
    return level


def gaussian(stream_key, shape, scale, most, split=(), held_as=jnp.bfloat16):
    drawn = scale * jax.random.normal(stream_key, shape, jnp.float32)
    if split:
        drawn = drawn * shard_levels(stream_key, shape, split, -0.22, 0.18)
    return jnp.clip(drawn, -most, most).astype(held_as)


def setup_inputs(seed: int = 0) -> dict:
    splits = jax.random.split(jax.random.key(seed), 7)
    return {
        "arriving": gaussian(splits[0], (SECTIONS, LENGTH, D), 1.0, 6.0, ((0, 8), (2, 32))),
        "norm_gain": jnp.clip(1.0 + 0.18 * jax.random.normal(splits[1], (SECTIONS, D), jnp.float32), 0.099609375, 1.8984375).astype(jnp.bfloat16),
        "w_query": draw_w_query(jax.random.fold_in(splits[6], 71), 0),
        "w_key": draw_w_key(jax.random.fold_in(splits[6], 71), 0),
        "w_value": gaussian(splits[4], (SECTIONS, KVD, D), (D // 16) ** -0.5, 0.25, ((0, 8), (1, 32))),
        "w_out": gaussian(splits[5], (SECTIONS, HEADS * HD, D), (HEADS * HD) ** -0.5, 0.0625, ((0, 8), (1, 32))),
    }


rope_base = 500000.0
norm_eps = 1e-05

def rotate(channel_major, first_channel):
    channels = channel_major.shape[0]
    length = channel_major.shape[1]
    within = (jnp.arange(channels, dtype=jnp.int32) + first_channel) % HD
    pair_index = (within // 2).astype(channel_major.dtype)
    frequency = jnp.exp(pair_index * (-2.0 * math.log(rope_base) / HD))
    positions = jnp.arange(length, dtype=jnp.int32).astype(channel_major.dtype)
    angles = frequency[0::2, None] * positions[None, :]
    cos_table = jnp.cos(angles)
    sine_table = jnp.sin(angles)
    paired = channel_major.reshape(channels // 2, 2, length)
    even_part = paired[:, 0]
    odd_part = paired[:, 1]
    rotated = jnp.stack([even_part * cos_table - odd_part * sine_table, even_part * sine_table + odd_part * cos_table], axis=1)
    return rotated.reshape(channels, length)

def head_order(pair_major):
    length = pair_major.shape[1]
    grouped = pair_major.reshape(HD // 2, KV_HEADS, 2, length)
    return jnp.transpose(grouped, (1, 0, 2, 3)).reshape(KV_HEADS * HD, length)

def normalize(hidden_in, gain_row):
    as_float = hidden_in.astype(jnp.float32)
    mean_square = lax.optimization_barrier(jnp.mean(as_float * as_float, axis=1, keepdims=True))
    normed = (as_float * lax.rsqrt(mean_square + norm_eps) * gain_row.astype(jnp.float32)).astype(jnp.bfloat16)
    return (as_float, normed)

def reference(arriving, norm_gain, w_query, w_key, w_value, w_out):
    group_size = HEADS // KV_HEADS
    width = HQ_DEV * HD
    score_scale = 1.0 / math.sqrt(HD)
    attended_all = []
    stream_all = []
    for section in range(SECTIONS):
        as_float, normed = normalize(arriving[(section - 1) % SECTIONS], norm_gain[section])
        length = normed.shape[0]
        queries = rotate(jnp.dot(w_query[section], normed.T, preferred_element_type=jnp.float32), 0).astype(jnp.bfloat16)
        key_all = rotate(head_order(jnp.dot(w_key[section], normed.T, preferred_element_type=jnp.float32)), 0).astype(jnp.bfloat16)
        value_all = head_order(jnp.dot(w_value[section], normed.T, preferred_element_type=jnp.float32)).astype(jnp.bfloat16)
        query_heads = queries.reshape(HEADS, HD, length).astype(jnp.float32)
        key_heads = jnp.repeat(key_all.reshape(KV_HEADS, HD, length), group_size, axis=0).astype(jnp.float32)
        value_heads = jnp.repeat(value_all.reshape(KV_HEADS, HD, length), group_size, axis=0).astype(jnp.float32)
        scores = jnp.einsum('hdi,hdj->hij', query_heads, key_heads) * score_scale
        token_index = jnp.arange(length, dtype=jnp.int32)
        causal = token_index[:, None] >= token_index[None, :]
        scores = jnp.where(causal[None], scores, -1e+30)
        row_max = lax.optimization_barrier(jnp.max(scores, axis=-1, keepdims=True))
        exponent = jnp.exp(scores - row_max)
        row_total = lax.optimization_barrier(jnp.sum(exponent, axis=-1, keepdims=True))
        weights = (exponent / row_total).astype(jnp.bfloat16)
        context = jnp.einsum('hij,hdj->ihd', weights.astype(jnp.float32), value_heads).astype(jnp.bfloat16)
        context = context.reshape(length, HEADS * HD)
        summed = jnp.zeros((length, D), jnp.float32)
        for shard in range(HEADS // HQ_DEV):
            partial_term = jnp.dot(context[:, shard * width:(shard + 1) * width], w_out[section][shard * width:(shard + 1) * width], preferred_element_type=jnp.float32)
            summed = summed + lax.optimization_barrier(partial_term.astype(jnp.bfloat16)).astype(jnp.float32)
        attended_all.append(summed.astype(jnp.bfloat16))
        stream_all.append((as_float + summed).astype(jnp.bfloat16))
    return (jnp.stack(attended_all), jnp.stack(stream_all))
```

```python
import functools
import math

import jax
import jax.numpy as jnp
from jax import lax
from jax.experimental import pallas as pl
from jax.experimental.pallas import tpu as pltpu
from jax.sharding import PartitionSpec as P

MESH = pl.DeviceIdType.MESH
BF16 = jnp.bfloat16
F32 = jnp.float32

X = 4
Z = 8
N = X * Z
SECTIONS = 8
LENGTH = 768
D = 8192
HD = 128
KV_HEADS = 8
WIDTH = D // N
ROWS = LENGTH // N
STREAMS = 4
QUARTER = LENGTH // STREAMS
PIECES = 4
PIECE = QUARTER // PIECES
SUMS = ROWS * D // 128 // STREAMS
SUM = SUMS // PIECES
QB = 256

ROPE_BASE = 500000.0
EPS = 1e-05


def spot(cycle, m):
    x, z = m // Z, lax.rem(m, Z)
    if cycle == 0:
        return X * z + lax.rem(x + z, X)
    b = lax.rem(z - 3 * x + 2 * Z, Z)
    return 4 * (x + X * (b // 4)) + lax.rem(b, 4)


def member(cycle, i):
    i = lax.rem(i, N)
    a, b = i // 4, lax.rem(i, 4)
    if cycle == 0:
        x, z = lax.rem(b - a + N, X), a
    else:
        x, z = lax.rem(a, X), lax.rem(3 * a + b, Z)
    return x * Z + z


def kernel(
    arriving, gain, w_query, w_key, w_value, w_out, cos_q, sin_q, turn_kv,
    attended, stream,
    hidden, wq, wkv_raw, wkv, wo, acc, squares, q_rot, own_kv, column_kv, all_kv, keys, values, context, term, landed,
    w_sem, shift_send, shift_recv, gather_send, gather_recv, x_send, x_recv, z_send, z_recv, scatter_send, scatter_recv,
):
    me = lax.axis_index("mp")
    section = lax.axis_index("section")
    x, z = me // Z, lax.rem(me, Z)
    cycles = [0, 0, 1, 1]
    forward = [True, False, True, False]
    places = [spot(c, me) for c in cycles]
    nexts = [
        member(c, p + (1 if f else N - 1)) for c, p, f in zip(cycles, places, forward)
    ]

    def behind(s, k):
        return member(cycles[s], places[s] + (N - k if forward[s] else k))

    loads = [
        pltpu.make_async_copy(w_key.at[0], wkv_raw.at[0], w_sem.at[0]),
        pltpu.make_async_copy(w_value.at[0], wkv_raw.at[1], w_sem.at[1]),
        pltpu.make_async_copy(w_query.at[0], wq, w_sem.at[2]),
        pltpu.make_async_copy(w_out.at[0], wo, w_sem.at[3]),
    ]
    for load in loads:
        load.start()

    barrier = pltpu.get_barrier_semaphore()
    for step in range(1, X):
        pl.semaphore_signal(
            barrier, inc=1, device_id={"mp": lax.rem(x + step, X) * Z + z}, device_id_type=MESH
        )
    for step in range(1, Z):
        pl.semaphore_signal(
            barrier, inc=1, device_id={"mp": x * Z + lax.rem(z + step, Z)}, device_id_type=MESH
        )
    for step in (1, SECTIONS - 1):
        pl.semaphore_signal(
            barrier, inc=1, device_id={"section": lax.rem(section + step, SECTIONS)}, device_id_type=MESH
        )
    pl.semaphore_wait(barrier, (X - 1) + (Z - 1) + 2)

    shifts = []
    for s in range(STREAMS):
        rows = pl.ds(s * QUARTER, QUARTER)
        shifts.append(
            pltpu.make_async_remote_copy(
                src_ref=arriving.at[0, rows],
                dst_ref=hidden.at[me, rows],
                send_sem=shift_send.at[s],
                recv_sem=shift_recv.at[s],
                device_id={"section": lax.rem(section + 1, SECTIONS)},
                device_id_type=MESH,
            )
        )
        shifts[-1].start()

    def pass_on(s, c, k, owner):
        part = hidden.at[owner, pl.ds(s * QUARTER + c * PIECE, PIECE)]
        return pltpu.make_async_remote_copy(
            src_ref=part,
            dst_ref=part,
            send_sem=gather_send.at[lax.rem(k, 2), s, c],
            recv_sem=gather_recv.at[k, s, c],
            device_id={"mp": nexts[s]},
            device_id_type=MESH,
        )

    def project(s, owner, first=False):
        rows = pl.ds(s * QUARTER, QUARTER)
        columns = pl.ds(pl.multiple_of(owner * WIDTH, WIDTH), WIDTH)
        block = hidden[owner, rows].astype(F32)
        squared = block * block
        squared = squared[:, :128] + squared[:, 128:]
        scaled = (block * gain[:, columns].astype(F32)).astype(BF16)
        contract = (((1,), (1,)), ((), ()))
        queries = lax.dot_general(scaled, wq[:, columns], contract, preferred_element_type=F32)
        others = lax.dot_general(scaled, wkv[:, columns], contract, preferred_element_type=F32)
        if first:
            squares[rows] = squared
            acc[rows, :WIDTH] = queries
            acc[rows, WIDTH:] = others
        else:
            squares[rows] += squared
            acc[rows, :WIDTH] += queries
            acc[rows, WIDTH:] += others

    for s in range(STREAMS):
        shifts[s].wait_recv()
        for c in range(PIECES):
            pass_on(s, c, 0, me).start()

    loads[0].wait()
    loads[1].wait()
    out_row = lax.broadcasted_iota(jnp.int32, (128, 64), 0)
    raw_row = lax.broadcasted_iota(jnp.int32, (128, 64), 1)
    head, j = lax.rem(out_row, 64) // 8, lax.rem(out_row, 8)
    channel = lax.rem(j, 4)
    turned = jnp.where(out_row >= 64, channel + 1 - 2 * lax.rem(channel, 2), channel)
    source = (j // 4) * 32 + (turned // 2) * 16 + head * 2 + lax.rem(turned, 2)
    pick = (raw_row == source).astype(F32).astype(BF16)
    for part in range(8):
        columns = pl.ds(part * (D // 8), D // 8)
        raw = jnp.concatenate([wkv_raw[0, :, columns], wkv_raw[1, :, columns]], axis=0)
        wkv[:, columns] = jnp.dot(pick, raw, preferred_element_type=F32).astype(BF16)
    loads[2].wait()
    for s in range(STREAMS):
        project(s, me, first=True)

    def gather_step(k, carry):
        for c in range(PIECES):
            for s in range(STREAMS):
                pass_on(s, c, k, behind(s, k + 1)).wait_recv()

                @pl.when(k >= 1)
                def _():
                    pass_on(s, c, k + 1, me).wait_send()

                pass_on(s, c, k + 1, behind(s, k + 1)).start()

            @pl.when(k >= 1)
            def _():
                project(c, behind(c, k))

        return carry

    lax.fori_loop(0, N - 2, gather_step, 0)
    for s in range(STREAMS):
        project(s, behind(s, N - 2))
    for s in range(STREAMS):
        for c in range(PIECES):
            pass_on(s, c, N - 2, behind(s, N - 1)).wait_recv()
        project(s, behind(s, N - 1))
    for s in range(STREAMS):
        for c in range(PIECES):
            pass_on(s, c, N - 3, me).wait_send()
            pass_on(s, c, N - 2, me).wait_send()
        shifts[s].wait_send()

    def scale_of(rows):
        mean = jnp.sum(squares[rows], axis=1, keepdims=True) * (1.0 / D)
        return lax.rsqrt(mean + EPS)

    for t in range(3):
        rows = pl.ds(t * QB, QB)
        both = acc[rows, WIDTH:] * scale_of(rows) * turn_kv[rows]
        ready = (both + pltpu.roll(both, 64, 1)).T
        for h in range(KV_HEADS):
            tile = ready[8 * h : 8 * h + 8]
            own_kv[h, t] = jnp.concatenate([tile[:, :128], tile[:, 128:]], axis=0).astype(BF16)

    x_copies = []
    for step in range(1, X):
        to = lax.rem(x + step, X)
        x_copies.append(
            pltpu.make_async_remote_copy(
                src_ref=own_kv.at[pl.ds(2 * to, 2)],
                dst_ref=column_kv.at[x],
                send_sem=x_send.at[step - 1],
                recv_sem=x_recv.at[step - 1],
                device_id={"mp": to * Z + z},
                device_id_type=MESH,
            )
        )
        x_copies[-1].start()
    for h in range(2):
        column_kv[x, h] = own_kv[2 * x + h]
    for copy in x_copies:
        copy.wait_recv()
    z_copies = []
    for step in range(1, Z):
        to = lax.rem(z + step, Z)
        z_copies.append(
            pltpu.make_async_remote_copy(
                src_ref=column_kv.at[:, to // 4],
                dst_ref=all_kv.at[:, z],
                send_sem=z_send.at[step - 1],
                recv_sem=z_recv.at[step - 1],
                device_id={"mp": x * Z + to},
                device_id_type=MESH,
            )
        )
        z_copies[-1].start()
    all_kv[:, z] = column_kv[:, z // 4]

    lane = lax.broadcasted_iota(jnp.int32, (QB, HD), 1)
    even = lax.rem(lane, 2) == 0
    for t in range(3):
        rows = pl.ds(t * QB, QB)
        scale = scale_of(rows)
        for h in range(2):
            query = acc[rows, h * HD : (h + 1) * HD] * scale
            swapped = jnp.where(even, pltpu.roll(query, HD - 1, 1), pltpu.roll(query, 1, 1))
            rotated = query * cos_q[rows] + swapped * sin_q[rows]
            q_rot[rows, h * HD : (h + 1) * HD] = rotated.astype(BF16)

    for copy in x_copies:
        copy.wait_send()
    for copy in z_copies:
        copy.wait()

    want = lax.broadcasted_iota(jnp.int32, (512, 512), 0)
    have = lax.broadcasted_iota(jnp.int32, (512, 512), 1)
    channel = lax.rem(want, 128)
    source = 16 * (channel // 4) + 4 * (want // 128) + lax.rem(channel, 4)
    pick = (have == source).astype(F32).astype(BF16)
    for t in range(3):
        arrived = all_kv[:, :, t].reshape(512, 128)
        sorted_rows = jnp.dot(pick, arrived, preferred_element_type=F32).astype(BF16)
        for half in range(2):
            columns = slice(t * QB + half * 128, t * QB + half * 128 + 128)
            keys[:, columns] = sorted_rows[256 * half : 256 * half + 128]
            values[:, columns] = sorted_rows[256 * half + 128 : 256 * half + 256]

    for t in range(3):
        rows = slice(t * QB, (t + 1) * QB)
        reach = (t + 1) * QB
        token = lax.broadcasted_iota(jnp.int32, (QB, reach), 0) + t * QB
        causal = token >= lax.broadcasted_iota(jnp.int32, (QB, reach), 1)
        for h in range(2):
            scores = jnp.dot(
                q_rot[rows, h * HD : (h + 1) * HD], keys[:, :reach], preferred_element_type=F32
            ) * (1.0 / math.sqrt(HD))
            scores = jnp.where(causal, scores, -1e30)
            exponent = jnp.exp(scores - jnp.max(scores, axis=1, keepdims=True))
            probs = (exponent / jnp.sum(exponent, axis=1, keepdims=True)).astype(BF16)
            mixed = lax.dot_general(
                probs, values[:, :reach], (((1,), (1,)), ((), ())), preferred_element_type=F32
            )
            context[rows, h * HD : (h + 1) * HD] = mixed.astype(BF16)

    def hand_on(s, c, k, owner):
        rows = pl.ds(s * SUMS + c * SUM, SUM)
        return pltpu.make_async_remote_copy(
            src_ref=term.at[owner, rows],
            dst_ref=landed.at[k, rows],
            send_sem=scatter_send.at[lax.rem(k, 2), s, c],
            recv_sem=scatter_recv.at[k, s, c],
            device_id={"mp": nexts[s]},
            device_id_type=MESH,
        )

    loads[3].wait()

    def project_out(tile):
        columns = pl.ds(pl.multiple_of(tile * 256, 256), 256)
        rows = pl.ds(pl.multiple_of(tile * 2 * ROWS, 2 * ROWS), 2 * ROWS)
        product = jnp.dot(context[...], wo[:, columns], preferred_element_type=F32)
        for owner in range(N):
            mine = product[owner * ROWS : (owner + 1) * ROWS]
            term[owner, rows] = jnp.concatenate([mine[:, :128], mine[:, 128:]], axis=0).astype(BF16)

    tiles = SUM // (2 * ROWS)
    for c in range(PIECES):

        def some(i, carry):
            s, u = i // tiles, lax.rem(i, tiles)
            project_out(s * (SUMS // (2 * ROWS)) + c * tiles + u)
            return carry

        lax.fori_loop(0, STREAMS * tiles, some, 0)
        for s in range(STREAMS):
            hand_on(s, c, 0, behind(s, 1)).start()

    def scatter_step(k, carry):
        for c in range(PIECES):
            for s in range(STREAMS):
                owner = behind(s, k + 2)
                rows = pl.ds(s * SUMS + c * SUM, SUM)
                hand_on(s, c, k, owner).wait_recv()

                @pl.when(k >= 1)
                def _():
                    hand_on(s, c, k + 1, owner).wait_send()

                total = term[owner, rows].astype(F32) + landed[k, rows].astype(F32)
                term[owner, rows] = total.astype(BF16)
                hand_on(s, c, k + 1, owner).start()
        return carry

    lax.fori_loop(0, N - 2, scatter_step, 0)

    first = me * ROWS
    offset = lax.rem(me, 2) * 8
    window = pl.ds(pl.multiple_of(first - offset, 16), ROWS + 8)

    for s in range(STREAMS):
        for c in range(PIECES):
            hand_on(s, c, N - 2, me).wait_recv()
            for u in range(tiles):
                at = s * SUMS + c * SUM + u * 2 * ROWS
                total = term[me, at : at + 2 * ROWS].astype(F32) + landed[N - 2, at : at + 2 * ROWS].astype(F32)
                owner = at // (2 * ROWS)
                total = jnp.concatenate([total[:ROWS], total[ROWS:]], axis=1)
                wide = hidden[owner, window].astype(F32)
                residual = jnp.where(offset == 0, wide[:ROWS], wide[8:])
                columns = slice(owner * WIDTH, (owner + 1) * WIDTH)
                attended[0, :, columns] = total.astype(BF16)
                stream[0, :, columns] = (residual + total).astype(BF16)
    for s in range(STREAMS):
        for c in range(PIECES):
            hand_on(s, c, N - 3, me).wait_send()
            hand_on(s, c, N - 2, me).wait_send()


def tables():
    member_id = lax.axis_index("mp")
    lanes = jnp.arange(HD, dtype=jnp.int32)
    positions = jnp.arange(LENGTH, dtype=jnp.int32).astype(F32)

    def angles(pairs):
        frequency = jnp.exp(pairs.astype(F32) * (-2.0 * math.log(ROPE_BASE) / HD))
        return positions[:, None] * frequency[None, :]

    sign = jnp.where(lanes % 2 == 0, -1.0, 1.0)
    turn = angles(lanes // 2)
    cos_q, sin_q = jnp.cos(turn), jnp.sin(turn) * sign
    j = lanes % 8
    turn = angles(2 * member_id + (j % 4) // 2)
    key_lane = j < 4
    turn_kv = jnp.where(
        lanes[None, :] < 64,
        jnp.where(key_lane, jnp.cos(turn), 1.0),
        jnp.where(key_lane, jnp.sin(turn) * sign, 0.0),
    )
    return cos_q, sin_q, turn_kv


def layer(arriving, norm_gain, w_query, w_key, w_value, w_out):
    any_space = pl.BlockSpec(memory_space=pl.ANY)
    vmem = pl.BlockSpec(memory_space=pltpu.VMEM)
    out = jax.ShapeDtypeStruct((1, ROWS, D), BF16)
    dma = pltpu.SemaphoreType.DMA
    return pl.pallas_call(
        kernel,
        out_shape=(out, out),
        in_specs=[vmem, vmem, any_space, any_space, any_space, any_space, vmem, vmem, vmem],
        out_specs=(vmem, vmem),
        scratch_shapes=[
            pltpu.VMEM((N, LENGTH, WIDTH), BF16),
            pltpu.VMEM((WIDTH, D), BF16),
            pltpu.VMEM((2, 32, D), BF16),
            pltpu.VMEM((128, D), BF16),
            pltpu.VMEM((WIDTH, D), BF16),
            pltpu.VMEM((LENGTH, WIDTH + 128), F32),
            pltpu.VMEM((LENGTH, 128), F32),
            pltpu.VMEM((LENGTH, WIDTH), BF16),
            pltpu.VMEM((KV_HEADS, 3, 16, 128), BF16),
            pltpu.VMEM((X, 2, 3, 16, 128), BF16),
            pltpu.VMEM((X, Z, 3, 16, 128), BF16),
            pltpu.VMEM((HD, LENGTH), BF16),
            pltpu.VMEM((HD, LENGTH), BF16),
            pltpu.VMEM((LENGTH, WIDTH), BF16),
            pltpu.VMEM((N, STREAMS * SUMS, 128), BF16),
            pltpu.VMEM((N - 1, STREAMS * SUMS, 128), BF16),
            dma((4,)),
            dma((STREAMS,)),
            dma((STREAMS,)),
            dma((2, STREAMS, PIECES)),
            dma((N - 1, STREAMS, PIECES)),
            dma((X - 1,)),
            dma((X - 1,)),
            dma((Z - 1,)),
            dma((Z - 1,)),
            dma((2, STREAMS, PIECES)),
            dma((N - 1, STREAMS, PIECES)),
        ],
        compiler_params=pltpu.CompilerParams(
            collective_id=0, has_side_effects=True, vmem_limit_bytes=67043328
        ),
    )(arriving, norm_gain, w_query, w_key, w_value, w_out, *tables())


def solution(mesh):
    return jax.shard_map(
        layer,
        mesh=mesh,
        in_specs=(
            P("section", None, "mp"),
            P("section", None),
            P("section", "mp", None),
            P("section", "mp", None),
            P("section", "mp", None),
            P("section", "mp", None),
        ),
        out_specs=(P("section", "mp", None), P("section", "mp", None)),
        check_vma=False,
    )
```

```python
import math

import jax
import jax.numpy as jnp
from jax import lax
from jax.experimental import pallas as pl
from jax.experimental.pallas import tpu as pltpu
from jax.sharding import PartitionSpec as P

MESH = pl.DeviceIdType.MESH
BF16 = jnp.bfloat16
F32 = jnp.float32

X = 4
Z = 8
N = X * Z
SECTIONS = 8
LENGTH = 768
D = 8192
HD = 128
KV_HEADS = 8
WIDTH = D // N
ROWS = LENGTH // N
UNIT = 2 * ROWS
QB = 256

ROPE_BASE = 500000.0
EPS = 1e-05

LINKS = ("x+", "x-", "z+", "z-")
STEP = {"x+": (1, 0), "x-": (-1, 0), "z+": (0, 1), "z-": (0, -1)}
OPPOSITE = {"x+": "x-", "x-": "x+", "z+": "z-", "z-": "z+"}
GATHER_CUTS = (0, 160, 320, 544, 768)
SCATTER_CUTS = (0, 6, 13, 23, 32)


def plan(cuts):
    a0, a1, a2, b1, b2 = cuts
    copies = {}
    for sign in (1, -1):
        x_link, z_link = ("x+", "z+") if sign == 1 else ("x-", "z-")
        half_a = (a0, a1) if sign == 1 else (a1, a2)
        half_b = (a2, b1) if sign == 1 else (b1, b2)
        copies[x_link, "A", 0] = ((), (a0, a2), (0, 0))
        copies[x_link, "A", 1] = (((x_link, "A", 0),), half_a, (-sign, 0))
        for o in (0, -1, 1, -2, 2, -3, 3, 4):
            if o == 0:
                wanted = ()
            elif o == 4:
                wanted = (("z+", "B", 3), ("z-", "B", 3))
            else:
                wanted = (("z+" if o < 0 else "z-", "B", abs(o) - 1),)
            copies[x_link, "B", o] = (wanted, (a2, b2), (0, o))
            copies[x_link, "C", o] = (((x_link, "B", o),), half_b, (-sign, o))
        for hop in range(4):
            wanted = ((z_link, "B", hop - 1),) if hop else ()
            copies[z_link, "B", hop] = (wanted, half_b if hop == 3 else (a2, b2), (0, -sign * hop))
        for i in (0, -1, 1, 2):
            first = {0: (), -1: (("x+", "A", 0),), 1: (("x-", "A", 0),), 2: (("x+", "A", 1), ("x-", "A", 1))}[i]
            for hop in range(4):
                wanted = ((z_link, "A", hop - 1, i),) if hop else first
                copies[z_link, "A", hop, i] = (wanted, half_a if hop == 3 else (a0, a2), (i, -sign * hop))
    return copies


def backwards(copies):
    after = {key: [] for key in copies}
    for key, (wanted, _, _) in copies.items():
        for other in wanted:
            after[other].append(key)
    return {key: (tuple(after[key]), rows, at) for key, (_, rows, at) in copies.items()}


def in_order(copies, bytes_per_row, rate=46.6e3, latency=2.5, queue=2):
    length = {key: (rows[1] - rows[0]) * bytes_per_row / rate for key, (_, rows, _) in copies.items()}
    after = backwards(copies)
    chain = {}

    def chain_of(key):
        if key not in chain:
            chain[key] = length[key] + max([chain_of(k) for k in after[key][0]], default=0.0)
        return chain[key]

    left, ready, queued = list(copies), {link: [] for link in LINKS}, {link: [] for link in LINKS}
    free = {link: 0.0 for link in LINKS}
    arrival, start, now = {}, {}, 0.0
    while left or any(ready.values()):
        for key in list(left):
            if all(k in arrival and arrival[k] <= now + 1e-9 for k in copies[key][0]):
                left.remove(key)
                ready[key[0]].append(key)
        for link in LINKS:
            queued[link] = [t for t in queued[link] if t > now + 1e-9]
            while ready[link] and len(queued[link]) < queue:
                key = max(ready[link], key=chain_of)
                ready[link].remove(key)
                start[key] = now
                free[link] = max(now, free[link]) + length[key]
                queued[link].append(free[link])
                arrival[key] = free[link] + latency
        times = [t for t in arrival.values() if t > now + 1e-9] + [t for q in queued.values() for t in q if t > now + 1e-9]
        now = min(times, default=now)
    return start, arrival


def seen_from_receiver(key, at):
    dx, dz = STEP[key[0]]
    return (at[0] - dx) % X, (at[1] - dz) % Z


GATHER = plan(GATHER_CUTS)
SCATTER = backwards(plan(SCATTER_CUTS))
KEYS = list(GATHER)
NUMBER = {key: n for n, key in enumerate(KEYS)}
SLOT = {}
LANDED = 0
for _key in KEYS:
    SLOT[_key] = LANDED
    LANDED += (SCATTER[_key][1][1] - SCATTER[_key][1][0]) * UNIT


def kernel(
    arriving, gain, w_query, w_key, w_value, w_out,
    attended, stream,
    hidden, wq, wkv_raw, wkv, wo, acc, squares, cos_q, sin_q, turn_kv, q_rot, own_kv, column_kv, all_kv, keys, values,
    context, term, landed,
    w_sem, shift_send, shift_recv, gather_send, gather_recv, x_send, x_recv, z_send, z_recv, scatter_send, scatter_recv,
):
    me = lax.axis_index("mp")
    section = lax.axis_index("section")
    x, z = me // Z, lax.rem(me, Z)

    def near(dx, dz):
        return lax.rem(x + dx % X, X) * Z + lax.rem(z + dz % Z, Z)

    loads = [
        pltpu.make_async_copy(w_key.at[0], wkv_raw.at[0], w_sem.at[0]),
        pltpu.make_async_copy(w_value.at[0], wkv_raw.at[1], w_sem.at[1]),
        pltpu.make_async_copy(w_query.at[0], wq, w_sem.at[2]),
        pltpu.make_async_copy(w_out.at[0], wo, w_sem.at[3]),
    ]
    for load in loads:
        load.start()

    barrier = pltpu.get_barrier_semaphore()
    for step in range(1, X):
        pl.semaphore_signal(barrier, inc=1, device_id={"mp": near(step, 0)}, device_id_type=MESH)
    for step in range(1, Z):
        pl.semaphore_signal(barrier, inc=1, device_id={"mp": near(0, step)}, device_id_type=MESH)
    for step in (1, SECTIONS - 1):
        pl.semaphore_signal(
            barrier, inc=1, device_id={"section": lax.rem(section + step, SECTIONS)}, device_id_type=MESH
        )
    pl.semaphore_wait(barrier, (X - 1) + (Z - 1) + 2)

    parts = (GATHER_CUTS[0], GATHER_CUTS[2], GATHER_CUTS[4])
    shifts = []
    for s in range(2):
        rows = pl.ds(parts[s], parts[s + 1] - parts[s])
        shifts.append(
            pltpu.make_async_remote_copy(
                src_ref=arriving.at[0, rows],
                dst_ref=hidden.at[me, rows],
                send_sem=shift_send.at[s],
                recv_sem=shift_recv.at[s],
                device_id={"section": lax.rem(section + 1, SECTIONS)},
                device_id_type=MESH,
            )
        )
        shifts[-1].start()

    loads[0].wait()
    loads[1].wait()
    out_row = lax.broadcasted_iota(jnp.int32, (128, 64), 0)
    raw_row = lax.broadcasted_iota(jnp.int32, (128, 64), 1)
    head, j = lax.rem(out_row, 64) // 8, lax.rem(out_row, 8)
    channel = lax.rem(j, 4)
    turned = jnp.where(out_row >= 64, channel + 1 - 2 * lax.rem(channel, 2), channel)
    source = (j // 4) * 32 + (turned // 2) * 16 + head * 2 + lax.rem(turned, 2)
    pick = (raw_row == source).astype(F32).astype(BF16)
    for part in range(8):
        columns = pl.ds(part * (D // 8), D // 8)
        raw = jnp.concatenate([wkv_raw[0, :, columns], wkv_raw[1, :, columns]], axis=0)
        wkv[:, columns] = jnp.dot(pick, raw, preferred_element_type=F32).astype(BF16)

    def passed(key):
        _, (low, high), at = GATHER[key]
        block = hidden.at[near(*at), pl.ds(low, high - low)]
        return pltpu.make_async_remote_copy(
            src_ref=block,
            dst_ref=block,
            send_sem=gather_send.at[NUMBER[key]],
            recv_sem=gather_recv.at[NUMBER[key]],
            device_id={"mp": near(*STEP[key[0]])},
            device_id_type=MESH,
        )

    def arrived_block(key):
        _, (low, high), at = GATHER[key]
        block = hidden.at[near(*seen_from_receiver(key, at)), pl.ds(low, high - low)]
        return pltpu.make_async_remote_copy(
            src_ref=block,
            dst_ref=block,
            send_sem=gather_send.at[NUMBER[key]],
            recv_sem=gather_recv.at[NUMBER[key]],
            device_id={"mp": near(*STEP[key[0]])},
            device_id_type=MESH,
        )

    started_rows = set()

    def project(part, at):
        owner = near(*at)
        rows = pl.ds(parts[part], parts[part + 1] - parts[part])
        columns = pl.ds(pl.multiple_of(owner * WIDTH, WIDTH), WIDTH)
        block = hidden[owner, rows].astype(F32)
        squared = block * block
        squared = squared[:, :128] + squared[:, 128:]
        scaled = (block * gain[:, columns].astype(F32)).astype(BF16)
        contract = (((1,), (1,)), ((), ()))
        queries = lax.dot_general(scaled, wq[:, columns], contract, preferred_element_type=F32)
        others = lax.dot_general(scaled, wkv[:, columns], contract, preferred_element_type=F32)
        if part not in started_rows:
            started_rows.add(part)
            squares[rows] = squared
            acc[rows, :WIDTH] = queries
            acc[rows, WIDTH:] = others
        else:
            squares[rows] += squared
            acc[rows, :WIDTH] += queries
            acc[rows, WIDTH:] += others

    def rotary_table(i):
        size = 64
        rows = pl.ds(i * size, size)
        lane = lax.broadcasted_iota(jnp.int32, (size, HD), 1)
        token = (lax.broadcasted_iota(jnp.int32, (size, HD), 0) + i * size).astype(F32)
        sign = jnp.where(lax.rem(lane, 2) == 0, -1.0, 1.0)

        def angle(pair):
            return token * jnp.exp(pair.astype(F32) * (-2.0 * math.log(ROPE_BASE) / HD))

        turn = angle(lane // 2)
        cos_q[rows] = jnp.cos(turn)
        sin_q[rows] = jnp.sin(turn) * sign
        j = lax.rem(lane, 8)
        turn = angle(2 * me + lax.rem(j, 4) // 2)
        stay = jnp.where(j < 4, jnp.cos(turn), 1.0)
        cross = jnp.where(j < 4, jnp.sin(turn) * sign, 0.0)
        turn_kv[rows] = jnp.where(lane < 64, stay, cross)

    start, arrival = in_order(GATHER, 2 * WIDTH)
    bringing = {((0, 0), 0): [], ((0, 0), 1): []}
    for key, (_, (low, _), at) in GATHER.items():
        bringing.setdefault((seen_from_receiver(key, at), int(low >= parts[1])), []).append(key)
    events = [(t, 0, "pass", key) for key, t in start.items()]
    events += [
        (max([arrival[k] for k in by], default=0.0) + (1.0 if by else 0.0), 1, "project", which)
        for which, by in bringing.items()
    ]
    events += [(3.0 + 1.5 * i, 2, "table", i) for i in range(12)]
    events.sort(key=lambda event: event[:2])
    waited = set()

    def need(key):
        if key not in waited:
            waited.add(key)
            arrived_block(key).wait_recv()

    shifts[0].wait_recv()
    shifts[1].wait_recv()
    query_weights_here = False
    for _, _, what, which in events:
        if what == "pass":
            for key in GATHER[which][0]:
                need(key)
            passed(which).start()
        elif what == "project":
            if not query_weights_here:
                query_weights_here = True
                loads[2].wait()
            for key in bringing[which]:
                need(key)
            project(which[1], which[0])
        else:
            rotary_table(which)

    def scale_of(rows):
        mean = jnp.sum(squares[rows], axis=1, keepdims=True) * (1.0 / D)
        return lax.rsqrt(mean + EPS)

    for t in range(3):
        rows = pl.ds(t * QB, QB)
        both = acc[rows, WIDTH:] * scale_of(rows) * turn_kv[rows]
        ready = (both + pltpu.roll(both, 64, 1)).T
        for h in range(KV_HEADS):
            tile = ready[8 * h : 8 * h + 8]
            own_kv[h, t] = jnp.concatenate([tile[:, :128], tile[:, 128:]], axis=0).astype(BF16)

    x_copies = []
    for step in range(1, X):
        to = lax.rem(x + step, X)
        x_copies.append(
            pltpu.make_async_remote_copy(
                src_ref=own_kv.at[pl.ds(2 * to, 2)],
                dst_ref=column_kv.at[x],
                send_sem=x_send.at[step - 1],
                recv_sem=x_recv.at[step - 1],
                device_id={"mp": near(step, 0)},
                device_id_type=MESH,
            )
        )
        x_copies[-1].start()
    for h in range(2):
        column_kv[x, h] = own_kv[2 * x + h]
    for copy in x_copies:
        copy.wait_recv()
    z_copies = []
    for step in range(1, Z):
        to = lax.rem(z + step, Z)
        z_copies.append(
            pltpu.make_async_remote_copy(
                src_ref=column_kv.at[:, to // 4],
                dst_ref=all_kv.at[:, z],
                send_sem=z_send.at[step - 1],
                recv_sem=z_recv.at[step - 1],
                device_id={"mp": near(0, step)},
                device_id_type=MESH,
            )
        )
        z_copies[-1].start()
    all_kv[:, z] = column_kv[:, z // 4]

    lane = lax.broadcasted_iota(jnp.int32, (QB, HD), 1)
    even = lax.rem(lane, 2) == 0
    for t in range(3):
        rows = pl.ds(t * QB, QB)
        scale = scale_of(rows)
        for h in range(2):
            query = acc[rows, h * HD : (h + 1) * HD] * scale
            swapped = jnp.where(even, pltpu.roll(query, HD - 1, 1), pltpu.roll(query, 1, 1))
            rotated = query * cos_q[rows] + swapped * sin_q[rows]
            q_rot[rows, h * HD : (h + 1) * HD] = rotated.astype(BF16)

    for key in KEYS:
        passed(key).wait_send()
    for shift in shifts:
        shift.wait_send()
    for copy in x_copies:
        copy.wait_send()
    for copy in z_copies:
        copy.wait()

    want = lax.broadcasted_iota(jnp.int32, (512, 512), 0)
    have = lax.broadcasted_iota(jnp.int32, (512, 512), 1)
    channel = lax.rem(want, 128)
    source = 16 * (channel // 4) + 4 * (want // 128) + lax.rem(channel, 4)
    pick = (have == source).astype(F32).astype(BF16)
    for t in range(3):
        arrived = all_kv[:, :, t].reshape(512, 128)
        sorted_rows = jnp.dot(pick, arrived, preferred_element_type=F32).astype(BF16)
        for half in range(2):
            columns = slice(t * QB + half * 128, t * QB + half * 128 + 128)
            keys[:, columns] = sorted_rows[256 * half : 256 * half + 128]
            values[:, columns] = sorted_rows[256 * half + 128 : 256 * half + 256]

    for t in range(3):
        rows = slice(t * QB, (t + 1) * QB)
        reach = (t + 1) * QB
        token = lax.broadcasted_iota(jnp.int32, (QB, reach), 0) + t * QB
        causal = token >= lax.broadcasted_iota(jnp.int32, (QB, reach), 1)
        for h in range(2):
            scores = jnp.dot(
                q_rot[rows, h * HD : (h + 1) * HD], keys[:, :reach], preferred_element_type=F32
            ) * (1.0 / math.sqrt(HD))
            scores = jnp.where(causal, scores, -1e30)
            exponent = jnp.exp(scores - jnp.max(scores, axis=1, keepdims=True))
            probs = (exponent / jnp.sum(exponent, axis=1, keepdims=True)).astype(BF16)
            mixed = lax.dot_general(
                probs, values[:, :reach], (((1,), (1,)), ((), ())), preferred_element_type=F32
            )
            context[rows, h * HD : (h + 1) * HD] = mixed.astype(BF16)

    def project_out(unit, carry):
        columns = pl.ds(pl.multiple_of(unit * 256, 256), 256)
        rows = pl.ds(pl.multiple_of(unit * UNIT, UNIT), UNIT)
        product = jnp.dot(context[...], wo[:, columns], preferred_element_type=F32)
        for owner in range(N):
            mine = product[owner * ROWS : (owner + 1) * ROWS]
            term[owner, rows] = jnp.concatenate([mine[:, :128], mine[:, 128:]], axis=0).astype(BF16)
        return carry

    def handed(key):
        _, (low, high), at = SCATTER[key]
        size = (high - low) * UNIT
        return pltpu.make_async_remote_copy(
            src_ref=term.at[near(*seen_from_receiver(key, at)), pl.ds(low * UNIT, size)],
            dst_ref=landed.at[pl.ds(SLOT[key], size)],
            send_sem=scatter_send.at[NUMBER[key]],
            recv_sem=scatter_recv.at[NUMBER[key]],
            device_id={"mp": near(*STEP[OPPOSITE[key[0]]])},
            device_id_type=MESH,
        )

    here = set()

    def landing(key):
        if key not in here:
            here.add(key)
            handed(key).wait_recv()

    loads[3].wait()
    done = set()
    start, _ = in_order(SCATTER, 2 * 128 * UNIT)
    for key in sorted(start, key=start.get):
        before, (low, high), at = SCATTER[key]
        missing = [u for u in range(low, high) if u not in done]
        if missing:
            done.update(missing)
            lax.fori_loop(missing[0], missing[-1] + 1, project_out, 0)
        for other in before:
            landing(other)
        if before:
            owner = near(*seen_from_receiver(key, at))
            edges = {low, high}
            for other in before:
                edges.update(e for e in SCATTER[other][1] if low < e < high)
            edges = sorted(edges)
            for a, b in zip(edges, edges[1:]):
                rows = pl.ds(a * UNIT, (b - a) * UNIT)
                total = term[owner, rows].astype(F32)
                for other in before:
                    l, h = SCATTER[other][1]
                    if l <= a and b <= h:
                        total += landed[pl.ds(SLOT[other] + (a - l) * UNIT, (b - a) * UNIT)].astype(F32)
                term[owner, rows] = total.astype(BF16)
        handed(key).start()

    first = me * ROWS
    offset = lax.rem(me, 2) * 8
    window = pl.ds(pl.multiple_of(first - offset, 16), ROWS + 8)
    last = [key for key in KEYS if not GATHER[key][0]]
    for unit in range(D // 256):
        total = term[me, unit * UNIT : (unit + 1) * UNIT].astype(F32)
        for key in last:
            low, high = SCATTER[key][1]
            if low <= unit < high:
                landing(key)
                at = SLOT[key] + (unit - low) * UNIT
                total += landed[at : at + UNIT].astype(F32)
        total = jnp.concatenate([total[:ROWS], total[ROWS:]], axis=1)
        wide = hidden[unit, window].astype(F32)
        residual = jnp.where(offset == 0, wide[:ROWS], wide[8:])
        columns = slice(unit * WIDTH, (unit + 1) * WIDTH)
        attended[0, :, columns] = total.astype(BF16)
        stream[0, :, columns] = (residual + total).astype(BF16)
    for key in KEYS:
        handed(key).wait_send()


def layer(arriving, norm_gain, w_query, w_key, w_value, w_out):
    any_space = pl.BlockSpec(memory_space=pl.ANY)
    vmem = pl.BlockSpec(memory_space=pltpu.VMEM)
    out = jax.ShapeDtypeStruct((1, ROWS, D), BF16)
    dma = pltpu.SemaphoreType.DMA
    return pl.pallas_call(
        kernel,
        out_shape=(out, out),
        in_specs=[vmem, vmem, any_space, any_space, any_space, any_space],
        out_specs=(vmem, vmem),
        scratch_shapes=[
            pltpu.VMEM((N, LENGTH, WIDTH), BF16),
            pltpu.VMEM((WIDTH, D), BF16),
            pltpu.VMEM((2, 32, D), BF16),
            pltpu.VMEM((128, D), BF16),
            pltpu.VMEM((WIDTH, D), BF16),
            pltpu.VMEM((LENGTH, WIDTH + 128), F32),
            pltpu.VMEM((LENGTH, 128), F32),
            pltpu.VMEM((LENGTH, HD), F32),
            pltpu.VMEM((LENGTH, HD), F32),
            pltpu.VMEM((LENGTH, HD), F32),
            pltpu.VMEM((LENGTH, WIDTH), BF16),
            pltpu.VMEM((KV_HEADS, 3, 16, 128), BF16),
            pltpu.VMEM((X, 2, 3, 16, 128), BF16),
            pltpu.VMEM((X, Z, 3, 16, 128), BF16),
            pltpu.VMEM((HD, LENGTH), BF16),
            pltpu.VMEM((HD, LENGTH), BF16),
            pltpu.VMEM((LENGTH, WIDTH), BF16),
            pltpu.VMEM((N, D // 128 * ROWS, 128), BF16),
            pltpu.VMEM((LANDED, 128), BF16),
            dma((4,)),
            dma((2,)),
            dma((2,)),
            dma((len(KEYS),)),
            dma((len(KEYS),)),
            dma((X - 1,)),
            dma((X - 1,)),
            dma((Z - 1,)),
            dma((Z - 1,)),
            dma((len(KEYS),)),
            dma((len(KEYS),)),
        ],
        compiler_params=pltpu.CompilerParams(
            collective_id=0, has_side_effects=True, vmem_limit_bytes=67043328
        ),
    )(arriving, norm_gain, w_query, w_key, w_value, w_out)


def solution(mesh):
    return jax.shard_map(
        layer,
        mesh=mesh,
        in_specs=(
            P("section", None, "mp"),
            P("section", None),
            P("section", "mp", None),
            P("section", "mp", None),
            P("section", "mp", None),
            P("section", "mp", None),
        ),
        out_specs=(P("section", "mp", None), P("section", "mp", None)),
        check_vma=False,
    )
```

```python
import math

import jax
import jax.numpy as jnp
from jax import lax
from jax.experimental import pallas as pl
from jax.experimental.pallas import tpu as pltpu
from jax.sharding import PartitionSpec as P

MESH = pl.DeviceIdType.MESH
BF16 = jnp.bfloat16
F32 = jnp.float32

X = 4
Z = 8
N = X * Z
SECTIONS = 8
LENGTH = 768
D = 8192
HD = 128
KV_HEADS = 8
WIDTH = D // N
ROWS = LENGTH // N
QB = 256
SPAN = ROWS * Z
TILE = 256
TILES = D // X // TILE
GROUPS = TILES // 2
BAND = X * ROWS

ROPE_BASE = 500000.0
EPS = 1e-05

LINKS = ("x+", "x-", "z+", "z-")
STEP = {"x+": (1, 0), "x-": (-1, 0), "z+": (0, 1), "z-": (0, -1)}
GATHER_CUTS = (0, 192, 384, 576, 768)
FAR_TILES = {"x+": (0, 1, 4, 5), "x-": (2, 3, 6, 7)}
NEAREST_LAST = (4, 3, -3, 2, -2, 1, -1, 0)


def plan(cuts):
    copies = {}
    n = 0
    a0, a1, a2, b1, b2 = cuts
    for sign in (1, -1):
        x_link, z_link = ("x+", "z+") if sign == 1 else ("x-", "z-")
        half_a = (a0, a1) if sign == 1 else (a1, a2)
        half_b = (a2, b1) if sign == 1 else (b1, b2)
        copies[x_link, n, "A", 0] = ((), (a0, a2), (0, 0))
        copies[x_link, n, "A", 1] = (((x_link, n, "A", 0),), half_a, (-sign, 0))
        for o in (0, -1, 1, -2, 2, -3, 3, 4):
            if o == 0:
                wanted = ()
            elif o == 4:
                wanted = (("z+", n, "B", 3), ("z-", n, "B", 3))
            else:
                wanted = (("z+" if o < 0 else "z-", n, "B", abs(o) - 1),)
            copies[x_link, n, "B", o] = (wanted, (a2, b2), (0, o))
            copies[x_link, n, "C", o] = (((x_link, n, "B", o),), half_b, (-sign, o))
        for hop in range(4):
            wanted = ((z_link, n, "B", hop - 1),) if hop else ()
            copies[z_link, n, "B", hop] = (wanted, half_b if hop == 3 else (a2, b2), (0, -sign * hop))
        for i in (0, -1, 1, 2):
            ends = (("x+", n, "A", 1), ("x-", n, "A", 1))
            first = {0: (), -1: (("x+", n, "A", 0),), 1: (("x-", n, "A", 0),), 2: ends}[i]
            for hop in range(4):
                wanted = ((z_link, n, "A", hop - 1, i),) if hop else first
                copies[z_link, n, "A", hop, i] = (wanted, half_a if hop == 3 else (a0, a2), (i, -sign * hop))
    return copies


def in_order(copies, ready_at, rate=46.6e3, latency=2.5, queue=2):
    length = {key: size / rate for key, (_, size) in copies.items()}
    after = {key: [] for key in copies}
    for key, (wanted, _) in copies.items():
        for other in wanted:
            after[other].append(key)
    chain = {}

    def chain_of(key):
        if key not in chain:
            chain[key] = length[key] + max([chain_of(k) for k in after[key]], default=0.0)
        return chain[key]

    left, ready, queued = list(copies), {link: [] for link in LINKS}, {link: [] for link in LINKS}
    free = {link: 0.0 for link in LINKS}
    arrival, start, now = {}, {}, 0.0
    while left or any(ready.values()):
        for key in list(left):
            if ready_at(key) <= now + 1e-9 and all(k in arrival and arrival[k] <= now + 1e-9 for k in copies[key][0]):
                left.remove(key)
                ready[key[0]].append(key)
        for link in LINKS:
            queued[link] = [t for t in queued[link] if t > now + 1e-9]
            while ready[link] and len(queued[link]) < queue:
                key = max(ready[link], key=lambda k: (-k[1], chain_of(k)))
                ready[link].remove(key)
                start[key] = now
                free[link] = max(now, free[link]) + length[key]
                queued[link].append(free[link])
                arrival[key] = free[link] + latency
        times = [t for t in arrival.values() if t > now + 1e-9] + [t for q in queued.values() for t in q if t > now + 1e-9]
        times += [ready_at(key) for key in left if ready_at(key) > now + 1e-9]
        now = min(times, default=now)
    return start, arrival


def seen_from_receiver(key, at):
    dx, dz = STEP[key[0]]
    return (at[0] - dx) % X, (at[1] - dz) % Z


GATHER = plan(GATHER_CUTS)
KEYS = list(GATHER)
NUMBER = {key: n for n, key in enumerate(KEYS)}


def kernel(
    arriving, gain, w_query, w_key, w_value, w_out,
    sums, entering,
    hidden, wq, wkv_raw, wkv, wo, stage, acc, squares, cos_q, sin_q, turn_kv, q_rot, own_kv, column_kv, all_kv, keys, values,
    own_context, context, term, landed, leaving, final,
    w_sem, wo_sem, shift_send, shift_recv, gather_send, gather_recv, weight_send, weight_recv, x_send, x_recv, z_send, z_recv,
    context_send, context_recv, scatter_send, scatter_recv, final_send, final_recv,
):
    me = lax.axis_index("mp")
    section = lax.axis_index("section")
    x, z = me // Z, lax.rem(me, Z)

    def near(dx, dz):
        return lax.rem(x + dx % X, X) * Z + lax.rem(z + dz % Z, Z)

    loads = [
        pltpu.make_async_copy(w_key.at[0], wkv_raw.at[0], w_sem.at[0]),
        pltpu.make_async_copy(w_value.at[0], wkv_raw.at[1], w_sem.at[1]),
        pltpu.make_async_copy(w_query.at[0], wq, w_sem.at[2]),
    ]

    def out_weights(place, tile):
        return w_out.at[0, :, pl.ds(pl.multiple_of(place * (D // X) + tile * TILE, TILE), TILE)]

    def from_place(place):
        return pl.ds(pl.multiple_of(place * WIDTH, WIDTH), WIDTH)

    for tile in range(TILES):
        loads.append(pltpu.make_async_copy(out_weights(x, tile), wo.at[tile, from_place(x)], wo_sem.at[tile]))
    for load in loads:
        load.start()

    barrier = pltpu.get_barrier_semaphore()
    for step in range(1, X):
        pl.semaphore_signal(barrier, inc=1, device_id={"mp": near(step, 0)}, device_id_type=MESH)
    for step in range(1, Z):
        pl.semaphore_signal(barrier, inc=1, device_id={"mp": near(0, step)}, device_id_type=MESH)
    for step in (1, SECTIONS - 1):
        pl.semaphore_signal(
            barrier, inc=1, device_id={"section": lax.rem(section + step, SECTIONS)}, device_id_type=MESH
        )
    pl.semaphore_wait(barrier, (X - 1) + (Z - 1) + 2)

    parts = (GATHER_CUTS[0:3:2], GATHER_CUTS[2:5:2])
    shifts = []
    for s, (low, high) in enumerate(parts):
        rows = pl.ds(low, high - low)
        shifts.append(
            pltpu.make_async_remote_copy(
                src_ref=arriving.at[0, rows],
                dst_ref=hidden.at[me, rows],
                send_sem=shift_send.at[s],
                recv_sem=shift_recv.at[s],
                device_id={"section": lax.rem(section + 1, SECTIONS)},
                device_id_type=MESH,
            )
        )
        shifts[-1].start()

    loads[0].wait()
    loads[1].wait()
    out_row = lax.broadcasted_iota(jnp.int32, (128, 64), 0)
    raw_row = lax.broadcasted_iota(jnp.int32, (128, 64), 1)
    head, j = lax.rem(out_row, 64) // 8, lax.rem(out_row, 8)
    channel = lax.rem(j, 4)
    turned = jnp.where(out_row >= 64, channel + 1 - 2 * lax.rem(channel, 2), channel)
    source = (j // 4) * 32 + (turned // 2) * 16 + head * 2 + lax.rem(turned, 2)
    pick = (raw_row == source).astype(F32).astype(BF16)
    for part in range(8):
        columns = pl.ds(part * (D // 8), D // 8)
        raw = jnp.concatenate([wkv_raw[0, :, columns], wkv_raw[1, :, columns]], axis=0)
        wkv[:, columns] = jnp.dot(pick, raw, preferred_element_type=F32).astype(BF16)

    def passed(key):
        _, (low, high), at = GATHER[key]
        block = hidden.at[near(*at), pl.ds(low, high - low)]
        return pltpu.make_async_remote_copy(
            src_ref=block,
            dst_ref=block,
            send_sem=gather_send.at[NUMBER[key]],
            recv_sem=gather_recv.at[NUMBER[key]],
            device_id={"mp": near(*STEP[key[0]])},
            device_id_type=MESH,
        )

    def weights(key):
        link, _, kind, i = key
        way = STEP[link][0]
        side = 0 if way == 1 else 1
        slot = {"W": 0, "V": TILES, "U": TILES + TILES // 2}[kind] + i
        if kind == "W":
            source, target = out_weights(lax.rem(x + way + X, X), i), wo.at[i, from_place(x)]
        elif kind == "V":
            source, target = out_weights(lax.rem(x + 2, X), FAR_TILES[link][i]), stage.at[side, i]
        else:
            source, target = stage.at[side, i], wo.at[FAR_TILES[link][i], from_place(lax.rem(x - way + X, X))]
        return pltpu.make_async_remote_copy(
            src_ref=source,
            dst_ref=target,
            send_sem=weight_send.at[side, slot],
            recv_sem=weight_recv.at[side, slot],
            device_id={"mp": near(way, 0)},
            device_id_type=MESH,
        )

    def arrived_block(key):
        _, (low, high), at = GATHER[key]
        block = hidden.at[near(*seen_from_receiver(key, at)), pl.ds(low, high - low)]
        return pltpu.make_async_remote_copy(
            src_ref=block,
            dst_ref=block,
            send_sem=gather_send.at[NUMBER[key]],
            recv_sem=gather_recv.at[NUMBER[key]],
            device_id={"mp": near(*STEP[key[0]])},
            device_id_type=MESH,
        )

    started_rows = set()

    def project(part, at):
        owner = near(*at)
        rows = pl.ds(parts[part][0], parts[part][1] - parts[part][0])
        columns = pl.ds(pl.multiple_of(owner * WIDTH, WIDTH), WIDTH)
        block = hidden[owner, rows].astype(F32)
        squared = block * block
        squared = squared[:, :128] + squared[:, 128:]
        scaled = (block * gain[:, columns].astype(F32)).astype(BF16)
        contract = (((1,), (1,)), ((), ()))
        queries = lax.dot_general(scaled, wq[:, columns], contract, preferred_element_type=F32)
        others = lax.dot_general(scaled, wkv[:, columns], contract, preferred_element_type=F32)
        if part not in started_rows:
            started_rows.add(part)
            squares[rows] = squared
            acc[rows, :WIDTH] = queries
            acc[rows, WIDTH:] = others
        else:
            squares[rows] += squared
            acc[rows, :WIDTH] += queries
            acc[rows, WIDTH:] += others

    def rotary_table(i):
        size = 64
        rows = pl.ds(i * size, size)
        lane = lax.broadcasted_iota(jnp.int32, (size, HD), 1)
        token = (lax.broadcasted_iota(jnp.int32, (size, HD), 0) + i * size).astype(F32)
        sign = jnp.where(lax.rem(lane, 2) == 0, -1.0, 1.0)

        def angle(pair):
            return token * jnp.exp(pair.astype(F32) * (-2.0 * math.log(ROPE_BASE) / HD))

        turn = angle(lane // 2)
        cos_q[rows] = jnp.cos(turn)
        sin_q[rows] = jnp.sin(turn) * sign
        j = lax.rem(lane, 8)
        turn = angle(2 * me + lax.rem(j, 4) // 2)
        stay = jnp.where(j < 4, jnp.cos(turn), 1.0)
        cross = jnp.where(j < 4, jnp.sin(turn) * sign, 0.0)
        turn_kv[rows] = jnp.where(lane < 64, stay, cross)

    def scale_of(rows):
        mean = jnp.sum(squares[rows], axis=1, keepdims=True) * (1.0 / D)
        return lax.rsqrt(mean + EPS)

    blocks = ((0, 1, 2),)
    x_copies, z_copies = {}, {}

    def send_along_x(n):
        for t in blocks[n]:
            rows = pl.ds(t * QB, QB)
            both = acc[rows, WIDTH:] * scale_of(rows) * turn_kv[rows]
            ready = (both + pltpu.roll(both, 64, 1)).T
            for h in range(KV_HEADS):
                tile = ready[8 * h : 8 * h + 8]
                own_kv[h, t] = jnp.concatenate([tile[:, :128], tile[:, 128:]], axis=0).astype(BF16)
        these = pl.ds(blocks[n][0], len(blocks[n]))
        for step in range(1, X):
            to = lax.rem(x + step, X)
            copy = pltpu.make_async_remote_copy(
                src_ref=own_kv.at[pl.ds(2 * to, 2), these],
                dst_ref=column_kv.at[x, :, these],
                send_sem=x_send.at[n, step - 1],
                recv_sem=x_recv.at[n, step - 1],
                device_id={"mp": near(step, 0)},
                device_id_type=MESH,
            )
            copy.start()
            x_copies[n, step] = copy
        for h in range(2):
            column_kv[x, h, these] = own_kv[2 * x + h, these]

    def send_along_z(n):
        these = pl.ds(blocks[n][0], len(blocks[n]))
        for step in range(1, X):
            x_copies[n, step].wait_recv()
        for step in range(1, Z):
            to = lax.rem(z + step, Z)
            copy = pltpu.make_async_remote_copy(
                src_ref=column_kv.at[:, to // 4, these],
                dst_ref=all_kv.at[:, z, these],
                send_sem=z_send.at[n, step - 1],
                recv_sem=z_recv.at[n, step - 1],
                device_id={"mp": near(0, step)},
                device_id_type=MESH,
            )
            copy.start()
            z_copies[n, step] = copy
        for t in blocks[n]:
            all_kv[:, z, t] = column_kv[:, z // 4, t]

    def turn_queries(t):
        lane = lax.broadcasted_iota(jnp.int32, (QB, HD), 1)
        even = lax.rem(lane, 2) == 0
        rows = pl.ds(t * QB, QB)
        scale = scale_of(rows)
        for h in range(2):
            query = acc[rows, h * HD : (h + 1) * HD] * scale
            swapped = jnp.where(even, pltpu.roll(query, HD - 1, 1), pltpu.roll(query, 1, 1))
            rotated = query * cos_q[rows] + swapped * sin_q[rows]
            q_rot[rows, h * HD : (h + 1) * HD] = rotated.astype(BF16)

    def sort_keys(n):
        for step in range(1, Z):
            z_copies[n, step].wait_recv()
        want = lax.broadcasted_iota(jnp.int32, (512, 512), 0)
        have = lax.broadcasted_iota(jnp.int32, (512, 512), 1)
        channel = lax.rem(want, 128)
        source = 16 * (channel // 4) + 4 * (want // 128) + lax.rem(channel, 4)
        pick = (have == source).astype(F32).astype(BF16)
        for t in blocks[n]:
            arrived = all_kv[:, :, t].reshape(512, 128)
            sorted_rows = jnp.dot(pick, arrived, preferred_element_type=F32).astype(BF16)
            for half in range(2):
                columns = slice(t * QB + half * 128, t * QB + half * 128 + 128)
                keys[:, columns] = sorted_rows[256 * half : 256 * half + 128]
                values[:, columns] = sorted_rows[256 * half + 128 : 256 * half + 256]

    def attend(t, h):
        rows = slice(t * SPAN, (t + 1) * SPAN)
        reach = -(-(t + 1) * SPAN // 128) * 128
        token = lax.broadcasted_iota(jnp.int32, (SPAN, reach), 0) + t * SPAN
        causal = token >= lax.broadcasted_iota(jnp.int32, (SPAN, reach), 1)
        scores = jnp.dot(
            q_rot[rows, h * HD : (h + 1) * HD], keys[:, :reach], preferred_element_type=F32
        ) * (1.0 / math.sqrt(HD))
        scores = jnp.where(causal, scores, -1e30)
        exponent = jnp.exp(scores - jnp.max(scores, axis=1, keepdims=True))
        probs = (exponent / jnp.sum(exponent, axis=1, keepdims=True)).astype(BF16)
        mixed = lax.dot_general(
            probs, values[:, :reach], (((1,), (1,)), ((), ())), preferred_element_type=F32
        )
        for place in range(Z):
            own_context[place, t * ROWS : (t + 1) * ROWS, h * HD : (h + 1) * HD] = mixed[place * ROWS : (place + 1) * ROWS]

    own_part = {("A", 0): 0, ("B", 0): 1, ("A", 0, 0): 0}
    own_at = (4.5, 7.0)
    copies = {key: (wanted, (rows[1] - rows[0]) * 2 * WIDTH) for key, (wanted, rows, _) in GATHER.items()}
    for link in ("x+", "x-"):
        for i in range(TILES // 2):
            copies[link, 1, "V", i] = ((), WIDTH * TILE * 2)
            copies[link, 1, "U", i] = (((link, 1, "V", i),), WIDTH * TILE * 2)

    def own_ready(key):
        return 0.0 if key[1] or GATHER[key][0] else own_at[own_part[key[2:]]]

    start, arrival = in_order(copies, own_ready)
    bringing = {((0, 0), part): [] for part in range(len(parts))}
    for key, (_, (low, _), at) in GATHER.items():
        part = int(low >= parts[1][0])
        bringing.setdefault((seen_from_receiver(key, at), part), []).append(key)
    events = [(t, 0, "weights" if key[1] else "pass", key) for key, t in start.items()]
    events += [
        (max([arrival[k] + 1.0 for k in by], default=own_at[which[1]] + 0.1), 1, "project", which)
        for which, by in bringing.items()
    ]
    events += [(5.0 + 1.5 * i, 2, "table", i) for i in range(12)]
    events.sort(key=lambda event: event[:2])
    waited = set()

    def need(key):
        if key not in waited:
            waited.add(key)
            (weights if key[1] else arrived_block)(key).wait_recv()

    def need_own(part):
        if ("own", part) not in waited:
            waited.add(("own", part))
            shifts[part].wait_recv()

    query_weights_here = False
    for _, _, what, which in events:
        if what == "pass":
            for key in GATHER[which][0]:
                need(key)
            if not GATHER[which][0]:
                need_own(own_part[which[2:]])
            passed(which).start()
        elif what == "project":
            if not query_weights_here:
                query_weights_here = True
                loads[2].wait()
            for key in bringing[which]:
                need(key)
            if not bringing[which]:
                need_own(which[1])
            project(which[1], which[0])
        elif what == "weights":
            for key in copies[which][0]:
                need(key)
            weights(which).start()
        else:
            rotary_table(which)

    send_along_x(0)
    for t in range(3):
        turn_queries(t)
    send_along_z(0)
    for i in range(TILES // 2):
        for link in ("x+", "x-"):
            weights((link, 1, "W", i)).start()
    for key in KEYS:
        passed(key).wait_send()
    for shift in shifts:
        shift.wait_send()
    first = me * ROWS
    offset = lax.rem(me, 2) * 8
    window = pl.ds(pl.multiple_of(first - offset, 16), ROWS + 8)
    for unit in range(N):
        wide = hidden[unit, window].astype(F32)
        residual = jnp.where(offset == 0, wide[:ROWS], wide[8:])
        entering[0, :, unit * WIDTH : (unit + 1) * WIDTH] = residual.astype(BF16)
    sort_keys(0)
    for t in range(X):
        for h in range(2):
            attend(t, h)
    for place in range(Z):
        context[x, place] = own_context[place].astype(BF16)
    for copy in list(x_copies.values()) + list(z_copies.values()):
        copy.wait_send()

    def hand_context(link, hop, i):
        way = STEP[link][0]
        side = 0 if way == 1 else 1
        place = lax.rem(z + NEAREST_LAST[i] + Z, Z)
        if hop == 0:
            part = context.at[x, place]
        else:
            part = context.at[lax.rem(x - way + X, X), place, pl.ds(side * (BAND // 2), BAND // 2)]
        return pltpu.make_async_remote_copy(
            src_ref=part,
            dst_ref=part,
            send_sem=context_send.at[side, hop, i],
            recv_sem=context_recv.at[side, hop, i],
            device_id={"mp": near(way, 0)},
            device_id_type=MESH,
        )

    def make_terms(i, half):
        place = lax.rem(z + NEAREST_LAST[i] + Z, Z)
        mixed = jnp.concatenate([context[c, place] for c in range(X)], axis=1)
        for tile in range(half * GROUPS, (half + 1) * GROUPS):
            product = jnp.dot(mixed, wo[tile], preferred_element_type=F32)
            columns = slice(tile % 2 * TILE, (tile % 2 + 1) * TILE)
            term[i, tile // 2, :, columns] = product.astype(BF16)

    def handed(way, step, group):
        side = 0 if way == 1 else 1
        return pltpu.make_async_remote_copy(
            src_ref=term.at[NEAREST_LAST.index(way * (4 - step) if step else 4), group],
            dst_ref=landed.at[side, step, group],
            send_sem=scatter_send.at[side, step, group],
            recv_sem=scatter_recv.at[side, step, group],
            device_id={"mp": near(0, way)},
            device_id_type=MESH,
        )

    def starts_here(way, step, group):
        return step == 0 or (step == 1 and group % 2 != (0 if way == 1 else 1))

    def hand_on(way, step, group):
        if not starts_here(way, step, group):
            handed(way, step - 1, group).wait_recv()
            i = NEAREST_LAST.index(way * (4 - step))
            total = term[i, group].astype(F32) + landed[0 if way == 1 else 1, step - 1, group].astype(F32)
            term[i, group] = total.astype(BF16)
        handed(way, step, group).start()

    def ready_ones(i, half):
        groups = (2 * half, 2 * half + 1)
        away = NEAREST_LAST[i]
        if away == 4:
            every = [(1, 0, groups[0]), (-1, 0, groups[1])]
        elif away == 0:
            every = []
        else:
            way = 1 if away > 0 else -1
            every = [(way, 4 - abs(away), g) for g in groups]
        now = [c for c in every if starts_here(*c)]
        later = [c for c in every if not starts_here(*c)]
        return now, sorted(later, key=lambda c: (c[2] % 2 == (0 if c[0] == 1 else 1)) if c[1] > 1 else 0)

    def leave(group, step):
        to = lax.rem(x + step, X)
        return pltpu.make_async_remote_copy(
            src_ref=leaving.at[to, group],
            dst_ref=final.at[x, group],
            send_sem=final_send.at[step - 1, group],
            recv_sem=final_recv.at[step - 1, group],
            device_id={"mp": near(step, 0)},
            device_id_type=MESH,
        )

    def finish(group):
        total = term[NEAREST_LAST.index(0), group].astype(F32)
        for way in (1, -1):
            handed(way, 3, group).wait_recv()
            total += landed[0 if way == 1 else 1, 3, group].astype(F32)
        for to in range(X):
            mine = total[to * ROWS : (to + 1) * ROWS]
            leaving[to, group] = jnp.concatenate([mine[:, :TILE], mine[:, TILE:]], axis=0).astype(BF16)
        for step in range(1, X):
            leave(group, step).start()
        final[x, group] = leaving[x, group]

    def write(group):
        for step in range(1, X):
            leave(group, step).wait_recv()
        for place in range(X):
            total = final[place, group].astype(F32)
            at = place * (D // X) + group * 2 * TILE
            sums[0, :, at : at + TILE] = total[:ROWS]
            sums[0, :, at + TILE : at + 2 * TILE] = total[ROWS:]

    def weights_of(half):
        for tile in range(half * GROUPS, (half + 1) * GROUPS):
            loads[3 + tile].wait()
            for link in ("x+", "x-"):
                need((link, 1, "W", tile))
                if tile in FAR_TILES[link]:
                    need((link, 1, "U", FAR_TILES[link].index(tile)))

    def pass_context(j):
        for link in ("x+", "x-"):
            hand_context(link, 0, j).wait_recv()
        for link in ("x+", "x-"):
            hand_context(link, 1, j).start()
            if j + 4 < Z:
                hand_context(link, 0, j + 4).start()

    for j in range(4):
        for link in ("x+", "x-"):
            hand_context(link, 0, j).start()
    pass_context(0)
    pass_context(1)
    weights_of(0)
    lagging = []
    for i in range(Z):
        for j in (2 * i + 2, 2 * i + 3):
            if j < Z:
                pass_context(j)
        if 2 * i + 3 == Z - 1:
            for tile in range(TILES // 2, TILES):
                for link in ("x+", "x-"):
                    weights((link, 1, "W", tile)).start()
        for link in ("x+", "x-"):
            hand_context(link, 1, i).wait_recv()
        make_terms(i, 0)
        now, later = ready_ones(i, 0)
        for copy in now + lagging:
            hand_on(*copy)
        lagging = later
    weights_of(1)
    for i in range(Z):
        make_terms(i, 1)
        now, later = ready_ones(i, 1)
        for copy in now + lagging:
            hand_on(*copy)
        lagging = later
        if i == 3:
            finish(1)
            finish(0)
        if i == 6:
            write(1)
            write(0)
    for copy in lagging:
        hand_on(*copy)
    finish(3)
    finish(2)

    write(3)
    write(2)
    for link in ("x+", "x-"):
        for i in range(TILES):
            weights((link, 1, "W", i)).wait_send()
        for i in range(TILES // 2):
            weights((link, 1, "V", i)).wait_send()
            weights((link, 1, "U", i)).wait_send()
        for i in range(Z):
            for hop in range(2):
                hand_context(link, hop, i).wait_send()
    for way in (1, -1):
        for group in range(GROUPS):
            for step in range(4):
                if step or group % 2 == (0 if way == 1 else 1):
                    handed(way, step, group).wait_send()
    for group in range(GROUPS):
        for step in range(1, X):
            leave(group, step).wait_send()


def layer(arriving, norm_gain, w_query, w_key, w_value, w_out):
    any_space = pl.BlockSpec(memory_space=pl.ANY)
    vmem = pl.BlockSpec(memory_space=pltpu.VMEM)
    sums = jax.ShapeDtypeStruct((1, ROWS, D), F32)
    entering = jax.ShapeDtypeStruct((1, ROWS, D), BF16)
    dma = pltpu.SemaphoreType.DMA
    summed, residual = pl.pallas_call(
        kernel,
        out_shape=(sums, entering),
        in_specs=[vmem, vmem, any_space, any_space, any_space, any_space],
        out_specs=(vmem, vmem),
        scratch_shapes=[
            pltpu.VMEM((N, LENGTH, WIDTH), BF16),
            pltpu.VMEM((WIDTH, D), BF16),
            pltpu.VMEM((2, 32, D), BF16),
            pltpu.VMEM((128, D), BF16),
            pltpu.VMEM((TILES, X * WIDTH, TILE), BF16),
            pltpu.VMEM((2, TILES // 2, WIDTH, TILE), BF16),
            pltpu.VMEM((LENGTH, WIDTH + 128), F32),
            pltpu.VMEM((LENGTH, 128), F32),
            pltpu.VMEM((LENGTH, HD), F32),
            pltpu.VMEM((LENGTH, HD), F32),
            pltpu.VMEM((LENGTH, HD), F32),
            pltpu.VMEM((LENGTH, WIDTH), BF16),
            pltpu.VMEM((KV_HEADS, 3, 16, 128), BF16),
            pltpu.VMEM((X, 2, 3, 16, 128), BF16),
            pltpu.VMEM((X, Z, 3, 16, 128), BF16),
            pltpu.VMEM((HD, LENGTH), BF16),
            pltpu.VMEM((HD, LENGTH), BF16),
            pltpu.VMEM((Z, BAND, WIDTH), F32),
            pltpu.VMEM((X, Z, BAND, WIDTH), BF16),
            pltpu.VMEM((Z, GROUPS, BAND, 2 * TILE), BF16),
            pltpu.VMEM((2, 4, GROUPS, BAND, 2 * TILE), BF16),
            pltpu.VMEM((X, GROUPS, 2 * ROWS, TILE), BF16),
            pltpu.VMEM((X, GROUPS, 2 * ROWS, TILE), BF16),
            dma((3,)),
            dma((TILES,)),
            dma((2,)),
            dma((2,)),
            dma((len(KEYS),)),
            dma((len(KEYS),)),
            dma((2, 2 * TILES)),
            dma((2, 2 * TILES)),
            dma((1, X - 1)),
            dma((1, X - 1)),
            dma((1, Z - 1)),
            dma((1, Z - 1)),
            dma((2, 2, Z)),
            dma((2, 2, Z)),
            dma((2, 4, GROUPS)),
            dma((2, 4, GROUPS)),
            dma((X - 1, GROUPS)),
            dma((X - 1, GROUPS)),
        ],
        compiler_params=pltpu.CompilerParams(
            collective_id=0, has_side_effects=True, vmem_limit_bytes=67043328
        ),
    )(arriving, norm_gain, w_query, w_key, w_value, w_out)
    return summed.astype(BF16), (residual.astype(F32) + summed).astype(BF16)


def solution(mesh):
    return jax.shard_map(
        layer,
        mesh=mesh,
        in_specs=(
            P("section", None, "mp"),
            P("section", None),
            P("section", "mp", None),
            P("section", "mp", None),
            P("section", "mp", None),
            P("section", "mp", None),
        ),
        out_specs=(P("section", "mp", None), P("section", "mp", None)),
        check_vma=False,
    )
```

```python
import math

import jax
import jax.numpy as jnp
from jax import lax
from jax.experimental import pallas as pl
from jax.experimental.pallas import tpu as pltpu
from jax.sharding import PartitionSpec as P

MESH = pl.DeviceIdType.MESH
BF16 = jnp.bfloat16
F32 = jnp.float32

X = 4
Z = 8
N = X * Z
SECTIONS = 8
LENGTH = 768
D = 8192
HD = 128
KV_HEADS = 8
WIDTH = D // N
ROWS = LENGTH // N
QB = 256
SPAN = ROWS * Z
TILE = 256
TILES = D // X // TILE
PAIRS = TILES // 2
BAND = X * ROWS

ROPE_BASE = 500000.0
EPS = 1e-05

LINKS = ("x+", "x-", "z+", "z-")
STEP = {"x+": (1, 0), "x-": (-1, 0), "z+": (0, 1), "z-": (0, -1)}
GATHER_CUTS = (0, 192, 384, 576, 768)
FAR_TILES = {"x+": (0, 2, 4, 6), "x-": (1, 3, 5, 7)}
EARLY_FAR = 4
NEAREST_LAST = (4, 3, -3, 2, -2, 1, -1, 0)


def plan(cuts):
    copies = {}
    n = 0
    a0, a1, a2, b1, b2 = cuts
    for sign in (1, -1):
        x_link, z_link = ("x+", "z+") if sign == 1 else ("x-", "z-")
        half_a = (a0, a1) if sign == 1 else (a1, a2)
        half_b = (a2, b1) if sign == 1 else (b1, b2)
        copies[x_link, n, "A", 0] = ((), (a0, a2), (0, 0))
        copies[x_link, n, "A", 1] = (((x_link, n, "A", 0),), half_a, (-sign, 0))
        for o in (0, -1, 1, -2, 2, -3, 3, 4):
            if o == 0:
                wanted = ()
            elif o == 4:
                wanted = (("z+", n, "B", 3), ("z-", n, "B", 3))
            else:
                wanted = (("z+" if o < 0 else "z-", n, "B", abs(o) - 1),)
            copies[x_link, n, "B", o] = (wanted, (a2, b2), (0, o))
            copies[x_link, n, "C", o] = (((x_link, n, "B", o),), half_b, (-sign, o))
        for hop in range(4):
            wanted = ((z_link, n, "B", hop - 1),) if hop else ()
            copies[z_link, n, "B", hop] = (wanted, half_b if hop == 3 else (a2, b2), (0, -sign * hop))
        for i in (0, -1, 1, 2):
            ends = (("x+", n, "A", 1), ("x-", n, "A", 1))
            first = {0: (), -1: (("x+", n, "A", 0),), 1: (("x-", n, "A", 0),), 2: ends}[i]
            for hop in range(4):
                wanted = ((z_link, n, "A", hop - 1, i),) if hop else first
                copies[z_link, n, "A", hop, i] = (wanted, half_a if hop == 3 else (a0, a2), (i, -sign * hop))
    return copies


def in_order(copies, ready_at, rate=46.6e3, latency=2.5, queue=2):
    length = {key: size / rate for key, (_, size) in copies.items()}
    after = {key: [] for key in copies}
    for key, (wanted, _) in copies.items():
        for other in wanted:
            after[other].append(key)
    chain = {}

    def chain_of(key):
        if key not in chain:
            chain[key] = length[key] + max([chain_of(k) for k in after[key]], default=0.0)
        return chain[key]

    left, ready, queued = list(copies), {link: [] for link in LINKS}, {link: [] for link in LINKS}
    free = {link: 0.0 for link in LINKS}
    arrival, start, now = {}, {}, 0.0
    while left or any(ready.values()):
        for key in list(left):
            if ready_at(key) <= now + 1e-9 and all(k in arrival and arrival[k] <= now + 1e-9 for k in copies[key][0]):
                left.remove(key)
                ready[key[0]].append(key)
        for link in LINKS:
            queued[link] = [t for t in queued[link] if t > now + 1e-9]
            while ready[link] and len(queued[link]) < queue:
                key = max(ready[link], key=lambda k: (-k[1], chain_of(k)))
                ready[link].remove(key)
                start[key] = now
                free[link] = max(now, free[link]) + length[key]
                queued[link].append(free[link])
                arrival[key] = free[link] + latency
        times = [t for t in arrival.values() if t > now + 1e-9] + [t for q in queued.values() for t in q if t > now + 1e-9]
        times += [ready_at(key) for key in left if ready_at(key) > now + 1e-9]
        now = min(times, default=now)
    return start, arrival


def seen_from_receiver(key, at):
    dx, dz = STEP[key[0]]
    return (at[0] - dx) % X, (at[1] - dz) % Z


GATHER = plan(GATHER_CUTS)
KEYS = list(GATHER)
NUMBER = {key: n for n, key in enumerate(KEYS)}


def kernel(
    arriving, gain, w_query, w_key, w_value, w_out,
    sums, entering,
    hidden, wq, wkv_raw, wkv, wo, stage, acc, squares, cos_q, sin_q, turn_kv, q_rot, own_kv, column_kv, all_kv, keys, values,
    own_context, context, term, landed, whole, leaving, final,
    w_sem, wo_sem, shift_send, shift_recv, gather_send, gather_recv, weight_send, weight_recv, x_send, x_recv, z_send, z_recv,
    context_send, context_recv, scatter_send, scatter_recv, final_send, final_recv,
):
    me = lax.axis_index("mp")
    section = lax.axis_index("section")
    x, z = me // Z, lax.rem(me, Z)

    def near(dx, dz):
        return lax.rem(x + dx % X, X) * Z + lax.rem(z + dz % Z, Z)

    loads = [
        pltpu.make_async_copy(w_key.at[0], wkv_raw.at[0], w_sem.at[0]),
        pltpu.make_async_copy(w_value.at[0], wkv_raw.at[1], w_sem.at[1]),
        pltpu.make_async_copy(w_query.at[0], wq, w_sem.at[2]),
    ]

    def out_weights(place, tile):
        return w_out.at[0, :, pl.ds(pl.multiple_of(place * (D // X) + tile * TILE, TILE), TILE)]

    def from_place(place):
        return pl.ds(pl.multiple_of(place * WIDTH, WIDTH), WIDTH)

    for tile in range(TILES):
        loads.append(pltpu.make_async_copy(out_weights(x, tile), wo.at[tile, from_place(x)], wo_sem.at[tile]))
    for load in loads:
        load.start()

    barrier = pltpu.get_barrier_semaphore()
    for step in range(1, X):
        pl.semaphore_signal(barrier, inc=1, device_id={"mp": near(step, 0)}, device_id_type=MESH)
    for step in range(1, Z):
        pl.semaphore_signal(barrier, inc=1, device_id={"mp": near(0, step)}, device_id_type=MESH)
    for step in (1, SECTIONS - 1):
        pl.semaphore_signal(
            barrier, inc=1, device_id={"section": lax.rem(section + step, SECTIONS)}, device_id_type=MESH
        )
    pl.semaphore_wait(barrier, (X - 1) + (Z - 1) + 2)

    parts = (GATHER_CUTS[0:3:2], GATHER_CUTS[2:5:2])
    shifts = []
    for s, (low, high) in enumerate(parts):
        rows = pl.ds(low, high - low)
        shifts.append(
            pltpu.make_async_remote_copy(
                src_ref=arriving.at[0, rows],
                dst_ref=hidden.at[me, rows],
                send_sem=shift_send.at[s],
                recv_sem=shift_recv.at[s],
                device_id={"section": lax.rem(section + 1, SECTIONS)},
                device_id_type=MESH,
            )
        )
        shifts[-1].start()

    loads[0].wait()
    loads[1].wait()
    out_row = lax.broadcasted_iota(jnp.int32, (128, 64), 0)
    raw_row = lax.broadcasted_iota(jnp.int32, (128, 64), 1)
    head, j = lax.rem(out_row, 64) // 8, lax.rem(out_row, 8)
    channel = lax.rem(j, 4)
    turned = jnp.where(out_row >= 64, channel + 1 - 2 * lax.rem(channel, 2), channel)
    source = (j // 4) * 32 + (turned // 2) * 16 + head * 2 + lax.rem(turned, 2)
    pick = (raw_row == source).astype(F32).astype(BF16)
    for part in range(8):
        columns = pl.ds(part * (D // 8), D // 8)
        raw = jnp.concatenate([wkv_raw[0, :, columns], wkv_raw[1, :, columns]], axis=0)
        wkv[:, columns] = jnp.dot(pick, raw, preferred_element_type=F32).astype(BF16)

    def passed(key):
        _, (low, high), at = GATHER[key]
        block = hidden.at[near(*at), pl.ds(low, high - low)]
        return pltpu.make_async_remote_copy(
            src_ref=block,
            dst_ref=block,
            send_sem=gather_send.at[NUMBER[key]],
            recv_sem=gather_recv.at[NUMBER[key]],
            device_id={"mp": near(*STEP[key[0]])},
            device_id_type=MESH,
        )

    def weights(key):
        link, _, kind, i = key
        way = STEP[link][0]
        side = 0 if way == 1 else 1
        slot = {"W": 0, "V": TILES, "U": TILES + TILES // 2}[kind] + i
        if kind == "W":
            source, target = out_weights(lax.rem(x + way + X, X), i), wo.at[i, from_place(x)]
        elif kind == "V":
            source, target = out_weights(lax.rem(x + 2, X), FAR_TILES[link][i]), stage.at[side, i]
        else:
            source, target = stage.at[side, i], wo.at[FAR_TILES[link][i], from_place(lax.rem(x - way + X, X))]
        return pltpu.make_async_remote_copy(
            src_ref=source,
            dst_ref=target,
            send_sem=weight_send.at[side, slot],
            recv_sem=weight_recv.at[side, slot],
            device_id={"mp": near(way, 0)},
            device_id_type=MESH,
        )

    def arrived_block(key):
        _, (low, high), at = GATHER[key]
        block = hidden.at[near(*seen_from_receiver(key, at)), pl.ds(low, high - low)]
        return pltpu.make_async_remote_copy(
            src_ref=block,
            dst_ref=block,
            send_sem=gather_send.at[NUMBER[key]],
            recv_sem=gather_recv.at[NUMBER[key]],
            device_id={"mp": near(*STEP[key[0]])},
            device_id_type=MESH,
        )

    started_rows = set()

    def project(part, at):
        owner = near(*at)
        rows = pl.ds(parts[part][0], parts[part][1] - parts[part][0])
        columns = pl.ds(pl.multiple_of(owner * WIDTH, WIDTH), WIDTH)
        block = hidden[owner, rows].astype(F32)
        squared = block * block
        squared = squared[:, :128] + squared[:, 128:]
        scaled = (block * gain[:, columns].astype(F32)).astype(BF16)
        contract = (((1,), (1,)), ((), ()))
        queries = lax.dot_general(scaled, wq[:, columns], contract, preferred_element_type=F32)
        others = lax.dot_general(scaled, wkv[:, columns], contract, preferred_element_type=F32)
        if part not in started_rows:
            started_rows.add(part)
            squares[rows] = squared
            acc[rows, :WIDTH] = queries
            acc[rows, WIDTH:] = others
        else:
            squares[rows] += squared
            acc[rows, :WIDTH] += queries
            acc[rows, WIDTH:] += others

    def rotary_table(i):
        size = 64
        rows = pl.ds(i * size, size)
        lane = lax.broadcasted_iota(jnp.int32, (size, HD), 1)
        token = (lax.broadcasted_iota(jnp.int32, (size, HD), 0) + i * size).astype(F32)
        sign = jnp.where(lax.rem(lane, 2) == 0, -1.0, 1.0)

        def angle(pair):
            return token * jnp.exp(pair.astype(F32) * (-2.0 * math.log(ROPE_BASE) / HD))

        turn = angle(lane // 2)
        cos_q[rows] = jnp.cos(turn)
        sin_q[rows] = jnp.sin(turn) * sign
        j = lax.rem(lane, 8)
        turn = angle(2 * me + lax.rem(j, 4) // 2)
        stay = jnp.where(j < 4, jnp.cos(turn), 1.0)
        cross = jnp.where(j < 4, jnp.sin(turn) * sign, 0.0)
        turn_kv[rows] = jnp.where(lane < 64, stay, cross)

    def scale_of(rows):
        mean = jnp.sum(squares[rows], axis=1, keepdims=True) * (1.0 / D)
        return lax.rsqrt(mean + EPS)

    blocks = ((0,), (1,), (2,))
    x_copies, z_copies = {}, {}

    def send_along_x(n):
        for t in blocks[n]:
            rows = pl.ds(t * QB, QB)
            both = acc[rows, WIDTH:] * scale_of(rows) * turn_kv[rows]
            ready = (both + pltpu.roll(both, 64, 1)).T
            for h in range(KV_HEADS):
                tile = ready[8 * h : 8 * h + 8]
                own_kv[h, t] = jnp.concatenate([tile[:, :128], tile[:, 128:]], axis=0).astype(BF16)
        these = pl.ds(blocks[n][0], len(blocks[n]))
        for step in range(1, X):
            to = lax.rem(x + step, X)
            copy = pltpu.make_async_remote_copy(
                src_ref=own_kv.at[pl.ds(2 * to, 2), these],
                dst_ref=column_kv.at[x, :, these],
                send_sem=x_send.at[n, step - 1],
                recv_sem=x_recv.at[n, step - 1],
                device_id={"mp": near(step, 0)},
                device_id_type=MESH,
            )
            copy.start()
            x_copies[n, step] = copy
        for h in range(2):
            column_kv[x, h, these] = own_kv[2 * x + h, these]

    def send_along_z(n):
        these = pl.ds(blocks[n][0], len(blocks[n]))
        for step in range(1, X):
            x_copies[n, step].wait_recv()
        for step in range(1, Z):
            to = lax.rem(z + step, Z)
            copy = pltpu.make_async_remote_copy(
                src_ref=column_kv.at[:, to // 4, these],
                dst_ref=all_kv.at[:, z, these],
                send_sem=z_send.at[n, step - 1],
                recv_sem=z_recv.at[n, step - 1],
                device_id={"mp": near(0, step)},
                device_id_type=MESH,
            )
            copy.start()
            z_copies[n, step] = copy
        for t in blocks[n]:
            all_kv[:, z, t] = column_kv[:, z // 4, t]

    def turn_queries(t):
        lane = lax.broadcasted_iota(jnp.int32, (QB, HD), 1)
        even = lax.rem(lane, 2) == 0
        rows = pl.ds(t * QB, QB)
        scale = scale_of(rows)
        for h in range(2):
            query = acc[rows, h * HD : (h + 1) * HD] * scale
            swapped = jnp.where(even, pltpu.roll(query, HD - 1, 1), pltpu.roll(query, 1, 1))
            rotated = query * cos_q[rows] + swapped * sin_q[rows]
            q_rot[rows, h * HD : (h + 1) * HD] = rotated.astype(BF16)

    def sort_keys(n):
        for step in range(1, Z):
            z_copies[n, step].wait_recv()
        want = lax.broadcasted_iota(jnp.int32, (512, 512), 0)
        have = lax.broadcasted_iota(jnp.int32, (512, 512), 1)
        channel = lax.rem(want, 128)
        source = 16 * (channel // 4) + 4 * (want // 128) + lax.rem(channel, 4)
        pick = (have == source).astype(F32).astype(BF16)
        for t in blocks[n]:
            arrived = all_kv[:, :, t].reshape(512, 128)
            sorted_rows = jnp.dot(pick, arrived, preferred_element_type=F32).astype(BF16)
            for half in range(2):
                columns = slice(t * QB + half * 128, t * QB + half * 128 + 128)
                keys[:, columns] = sorted_rows[256 * half : 256 * half + 128]
                values[:, columns] = sorted_rows[256 * half + 128 : 256 * half + 256]

    def attend(t, h):
        rows = slice(t * SPAN, (t + 1) * SPAN)
        reach = -(-(t + 1) * SPAN // 128) * 128
        token = lax.broadcasted_iota(jnp.int32, (SPAN, reach), 0) + t * SPAN
        causal = token >= lax.broadcasted_iota(jnp.int32, (SPAN, reach), 1)
        scores = jnp.dot(
            q_rot[rows, h * HD : (h + 1) * HD], keys[:, :reach], preferred_element_type=F32
        ) * (1.0 / math.sqrt(HD))
        scores = jnp.where(causal, scores, -1e30)
        exponent = jnp.exp(scores - jnp.max(scores, axis=1, keepdims=True))
        probs = (exponent / jnp.sum(exponent, axis=1, keepdims=True)).astype(BF16)
        mixed = lax.dot_general(
            probs, values[:, :reach], (((1,), (1,)), ((), ())), preferred_element_type=F32
        )
        for place in range(Z):
            own_context[place, t * ROWS : (t + 1) * ROWS, h * HD : (h + 1) * HD] = mixed[place * ROWS : (place + 1) * ROWS]

    own_part = {("A", 0): 0, ("B", 0): 1, ("A", 0, 0): 0}
    own_at = (4.5, 7.0)
    copies = {key: (wanted, (rows[1] - rows[0]) * 2 * WIDTH) for key, (wanted, rows, _) in GATHER.items()}
    for link in ("x+", "x-"):
        for i in range(EARLY_FAR):
            copies[link, 1, "V", i] = ((), WIDTH * TILE * 2)
            copies[link, 1, "U", i] = (((link, 1, "V", i),), WIDTH * TILE * 2)

    def own_ready(key):
        return 0.0 if key[1] or GATHER[key][0] else own_at[own_part[key[2:]]]

    start, arrival = in_order(copies, own_ready)
    bringing = {((0, 0), part): [] for part in range(len(parts))}
    for key, (_, (low, _), at) in GATHER.items():
        part = int(low >= parts[1][0])
        bringing.setdefault((seen_from_receiver(key, at), part), []).append(key)
    events = [(t, 0, "weights" if key[1] else "pass", key) for key, t in start.items()]
    events += [
        (max([arrival[k] + 1.0 for k in by], default=own_at[which[1]] + 0.1), 1, "project", which)
        for which, by in bringing.items()
    ]
    events += [(5.0 + 1.5 * i, 2, "table", i) for i in range(12)]
    events.sort(key=lambda event: event[:2])
    waited = set()

    def need(key):
        if key not in waited:
            waited.add(key)
            (weights if key[1] else arrived_block)(key).wait_recv()

    def need_own(part):
        if ("own", part) not in waited:
            waited.add(("own", part))
            shifts[part].wait_recv()

    query_weights_here = False
    for _, _, what, which in events:
        if what == "pass":
            for key in GATHER[which][0]:
                need(key)
            if not GATHER[which][0]:
                need_own(own_part[which[2:]])
            passed(which).start()
        elif what == "project":
            if not query_weights_here:
                query_weights_here = True
                loads[2].wait()
            for key in bringing[which]:
                need(key)
            if not bringing[which]:
                need_own(which[1])
            project(which[1], which[0])
        elif what == "weights":
            for key in copies[which][0]:
                need(key)
            weights(which).start()
        else:
            rotary_table(which)

    for t in range(3):
        send_along_x(t)
    for t in range(3):
        turn_queries(t)
    for t in range(3):
        send_along_z(t)
    for i in range(TILES // 2):
        for link in ("x+", "x-"):
            weights((link, 1, "W", i)).start()
    for i in range(EARLY_FAR, TILES // 2):
        for link in ("x+", "x-"):
            weights((link, 1, "V", i)).start()
    for key in KEYS:
        passed(key).wait_send()
    for shift in shifts:
        shift.wait_send()
    first = me * ROWS
    offset = lax.rem(me, 2) * 8
    window = pl.ds(pl.multiple_of(first - offset, 16), ROWS + 8)
    for unit in range(N):
        wide = hidden[unit, window].astype(F32)
        residual = jnp.where(offset == 0, wide[:ROWS], wide[8:])
        entering[0, :, unit * WIDTH : (unit + 1) * WIDTH] = residual.astype(BF16)
    for t in range(X):
        if t < 3:
            sort_keys(t)
        for h in range(2):
            attend(t, h)
    for place in range(Z):
        context[x, place] = own_context[place].astype(BF16)
    for copy in list(x_copies.values()) + list(z_copies.values()):
        copy.wait_send()

    def hand_context(link, hop, i):
        way = STEP[link][0]
        side = 0 if way == 1 else 1
        place = lax.rem(z + NEAREST_LAST[i] + Z, Z)
        if hop == 0:
            part = context.at[x, place]
        else:
            part = context.at[lax.rem(x - way + X, X), place, pl.ds(side * (BAND // 2), BAND // 2)]
        return pltpu.make_async_remote_copy(
            src_ref=part,
            dst_ref=part,
            send_sem=context_send.at[side, hop, i],
            recv_sem=context_recv.at[side, hop, i],
            device_id={"mp": near(way, 0)},
            device_id_type=MESH,
        )

    def place_of(i):
        return lax.rem(z + NEAREST_LAST[i] + Z, Z)

    made = set()

    def make_terms(i, tile):
        if (i, tile) in made:
            return
        these = [n for n, away in enumerate(NEAREST_LAST) if abs(away) == abs(NEAREST_LAST[i])]
        made.update((n, tile) for n in these)
        for n in these:
            for link in ("x+", "x-"):
                need_late((link, "Q", n))
        if tile not in made:
            made.add(tile)
            loads[3 + tile].wait()
            for link in ("x+", "x-"):
                need_late((link, "W", tile))
                if tile in FAR_TILES[link]:
                    need_late((link, "U", FAR_TILES[link].index(tile)))
        mixed = [jnp.concatenate([context[c, place_of(n)] for c in range(X)], axis=1) for n in these]
        product = jnp.dot(jnp.concatenate(mixed, axis=0), wo[tile], preferred_element_type=F32).astype(BF16)
        for m, n in enumerate(these):
            term[n, tile] = product[m * BAND : (m + 1) * BAND]

    def handed(way, step, tile):
        side = 0 if way == 1 else 1
        return pltpu.make_async_remote_copy(
            src_ref=term.at[NEAREST_LAST.index(way * (4 - step) if step else 4), tile],
            dst_ref=landed.at[side, step, tile],
            send_sem=scatter_send.at[side, step, tile],
            recv_sem=scatter_recv.at[side, step, tile],
            device_id={"mp": near(0, way)},
            device_id_type=MESH,
        )

    def starts_here(way, step, tile):
        return step == 0 or (step == 1 and tile % 2 != (0 if way == 1 else 1))

    def hand_on(way, step, tile):
        if not starts_here(way, step, tile):
            handed(way, step - 1, tile).wait_recv()
            i = NEAREST_LAST.index(way * (4 - step))
            total = term[i, tile].astype(F32) + landed[0 if way == 1 else 1, step - 1, tile].astype(F32)
            term[i, tile] = total.astype(BF16)
        handed(way, step, tile).start()

    def leave(pair, step):
        to = lax.rem(x + step, X)
        return pltpu.make_async_remote_copy(
            src_ref=leaving.at[to, pair],
            dst_ref=final.at[x, pair],
            send_sem=final_send.at[step - 1, pair],
            recv_sem=final_recv.at[step - 1, pair],
            device_id={"mp": near(step, 0)},
            device_id_type=MESH,
        )

    def finish(pair):
        for tile in (2 * pair, 2 * pair + 1):
            make_terms(NEAREST_LAST.index(0), tile)
            total = term[NEAREST_LAST.index(0), tile].astype(F32)
            for way in (1, -1):
                handed(way, 3, tile).wait_recv()
                total += landed[0 if way == 1 else 1, 3, tile].astype(F32)
            whole[tile % 2] = total
        for to in range(X):
            rows = slice(to * ROWS, (to + 1) * ROWS)
            leaving[to, pair] = jnp.concatenate([whole[0, rows], whole[1, rows]], axis=0).astype(BF16)
        for step in range(1, X):
            leave(pair, step).start()
        final[x, pair] = leaving[x, pair]

    def write(pair):
        for step in range(1, X):
            leave(pair, step).wait_recv()
        for place in range(X):
            total = final[place, pair].astype(F32)
            at = place * (D // X) + pair * 2 * TILE
            sums[0, :, at : at + TILE] = total[:ROWS]
            sums[0, :, at + TILE : at + 2 * TILE] = total[ROWS:]

    late = {}
    late_tiles = {}
    for link in ("x+", "x-"):
        for i in range(Z):
            late[link, 0, "P", i] = ((), BAND * WIDTH * 2)
            late[link, 0, "Q", i] = (((link, 0, "P", i),), BAND * WIDTH)
        for tile in range(TILES // 2, TILES):
            key = (link, tile // 2 - 1, "W", tile)
            late[key] = ((), WIDTH * TILE * 2)
            late_tiles.setdefault(tile, []).append(key)
        for i in range(EARLY_FAR, TILES // 2):
            tile = FAR_TILES[link][i]
            key = (link, tile // 2 - 1, "U", i)
            late[key] = ((), WIDTH * TILE * 2)
            late_tiles.setdefault(tile, []).append(key)
    for way, link in ((1, "z+"), (-1, "z-")):
        for tile in range(TILES):
            rank = max(tile // 2 - 1, 0)
            for step in range(4):
                if step == 0 and starts_here(way, 1, tile):
                    continue
                away = way * (4 - step) if step else 4
                wanted = [(l, 0, "Q", n) for l in ("x+", "x-") for n, a in enumerate(NEAREST_LAST) if abs(a) == abs(away)]
                wanted += late_tiles.get(tile, [])
                if not starts_here(way, step, tile):
                    wanted.append((link, rank, "S", tile, step - 1))
                late[link, rank, "S", tile, step] = (tuple(wanted), BAND * TILE * 2)
    start, arrival = in_order(late, lambda key: 0.0)
    here = set()

    def need_late(key):
        if key not in here:
            here.add(key)
            link, kind, i = key
            if kind in "PQ":
                hand_context(link, 0 if kind == "P" else 1, i).wait_recv()
            else:
                need((link, 1, kind, i))

    events = [(t, 0, "copy", key) for key, t in start.items()]
    for pair in range(PAIRS):
        tiles = (2 * pair, 2 * pair + 1)
        there = max(arrival[link, max(pair - 1, 0), "S", tile, 3] for link in ("z+", "z-") for tile in tiles)
        events += [(there + 0.5, 1, "finish", pair), (there + 6.5, 2, "write", pair)]
    events.sort(key=lambda event: event[:2])
    for _, _, what, which in events:
        if what == "finish":
            finish(which)
        elif what == "write":
            write(which)
        elif which[2] == "P":
            hand_context(which[0], 0, which[3]).start()
        elif which[2] == "Q":
            need_late((which[0], "P", which[3]))
            hand_context(which[0], 1, which[3]).start()
        elif which[2] in "WU":
            if which[2] == "U":
                need((which[0], 1, "V", which[3]))
            weights((which[0], 1, which[2], which[3])).start()
        else:
            link, _, _, tile, step = which
            way = 1 if link == "z+" else -1
            make_terms(NEAREST_LAST.index(way * (4 - step) if step else 4), tile)
            hand_on(way, step, tile)

    for link in ("x+", "x-"):
        for i in range(TILES):
            weights((link, 1, "W", i)).wait_send()
        for i in range(TILES // 2):
            weights((link, 1, "V", i)).wait_send()
            weights((link, 1, "U", i)).wait_send()
        for i in range(Z):
            for hop in range(2):
                hand_context(link, hop, i).wait_send()
    for way in (1, -1):
        for tile in range(TILES):
            for step in range(4):
                if step or tile % 2 == (0 if way == 1 else 1):
                    handed(way, step, tile).wait_send()
    for pair in range(PAIRS):
        for step in range(1, X):
            leave(pair, step).wait_send()


def layer(arriving, norm_gain, w_query, w_key, w_value, w_out):
    any_space = pl.BlockSpec(memory_space=pl.ANY)
    vmem = pl.BlockSpec(memory_space=pltpu.VMEM)
    sums = jax.ShapeDtypeStruct((1, ROWS, D), F32)
    entering = jax.ShapeDtypeStruct((1, ROWS, D), BF16)
    dma = pltpu.SemaphoreType.DMA
    summed, residual = pl.pallas_call(
        kernel,
        out_shape=(sums, entering),
        in_specs=[vmem, vmem, any_space, any_space, any_space, any_space],
        out_specs=(vmem, vmem),
        scratch_shapes=[
            pltpu.VMEM((N, LENGTH, WIDTH), BF16),
            pltpu.VMEM((WIDTH, D), BF16),
            pltpu.VMEM((2, 32, D), BF16),
            pltpu.VMEM((128, D), BF16),
            pltpu.VMEM((TILES, X * WIDTH, TILE), BF16),
            pltpu.VMEM((2, TILES // 2, WIDTH, TILE), BF16),
            pltpu.VMEM((LENGTH, WIDTH + 128), F32),
            pltpu.VMEM((LENGTH, 128), F32),
            pltpu.VMEM((LENGTH, HD), F32),
            pltpu.VMEM((LENGTH, HD), F32),
            pltpu.VMEM((LENGTH, HD), F32),
            pltpu.VMEM((LENGTH, WIDTH), BF16),
            pltpu.VMEM((KV_HEADS, 3, 16, 128), BF16),
            pltpu.VMEM((X, 2, 3, 16, 128), BF16),
            pltpu.VMEM((X, Z, 3, 16, 128), BF16),
            pltpu.VMEM((HD, LENGTH), BF16),
            pltpu.VMEM((HD, LENGTH), BF16),
            pltpu.VMEM((Z, BAND, WIDTH), F32),
            pltpu.VMEM((X, Z, BAND, WIDTH), BF16),
            pltpu.VMEM((Z, TILES, BAND, TILE), BF16),
            pltpu.VMEM((2, 4, TILES, BAND, TILE), BF16),
            pltpu.VMEM((2, BAND, TILE), F32),
            pltpu.VMEM((X, PAIRS, 2 * ROWS, TILE), BF16),
            pltpu.VMEM((X, PAIRS, 2 * ROWS, TILE), BF16),
            dma((3,)),
            dma((TILES,)),
            dma((2,)),
            dma((2,)),
            dma((len(KEYS),)),
            dma((len(KEYS),)),
            dma((2, 2 * TILES)),
            dma((2, 2 * TILES)),
            dma((3, X - 1)),
            dma((3, X - 1)),
            dma((3, Z - 1)),
            dma((3, Z - 1)),
            dma((2, 2, Z)),
            dma((2, 2, Z)),
            dma((2, 4, TILES)),
            dma((2, 4, TILES)),
            dma((X - 1, PAIRS)),
            dma((X - 1, PAIRS)),
        ],
        compiler_params=pltpu.CompilerParams(
            collective_id=0, has_side_effects=True, vmem_limit_bytes=67043328
        ),
    )(arriving, norm_gain, w_query, w_key, w_value, w_out)
    return summed.astype(BF16), (residual.astype(F32) + summed).astype(BF16)


def solution(mesh):
    return jax.shard_map(
        layer,
        mesh=mesh,
        in_specs=(
            P("section", None, "mp"),
            P("section", None),
            P("section", "mp", None),
            P("section", "mp", None),
            P("section", "mp", None),
            P("section", "mp", None),
        ),
        out_specs=(P("section", "mp", None), P("section", "mp", None)),
        check_vma=False,
    )
```

```python
import math

import jax
import jax.numpy as jnp
from jax import lax
from jax.experimental import pallas as pl
from jax.experimental.pallas import tpu as pltpu
from jax.sharding import PartitionSpec as P

MESH = pl.DeviceIdType.MESH
BF16 = jnp.bfloat16
F32 = jnp.float32

X = 4
Z = 8
N = X * Z
SECTIONS = 8
LENGTH = 768
D = 8192
HD = 128
KV_HEADS = 8
WIDTH = D // N
ROWS = LENGTH // N
QB = 256
SPAN = ROWS * Z
TILE = 256
TILES = D // X // TILE
PAIRS = TILES // 2
BAND = X * ROWS

ROPE_BASE = 500000.0
EPS = 1e-05

LINKS = ("x+", "x-", "z+", "z-")
STEP = {"x+": (1, 0), "x-": (-1, 0), "z+": (0, 1), "z-": (0, -1)}
GATHER_CUTS = (0, 192, 384, 576, 768)
FAR_TILES = {"x+": (0, 2, 4, 6), "x-": (1, 3, 5, 7)}
EARLY_FAR = 4
NEAREST_LAST = (4, 3, -3, 2, -2, 1, -1, 0)


def plan(cuts):
    copies = {}
    n = 0
    a0, a1, a2, b1, b2 = cuts
    for sign in (1, -1):
        x_link, z_link = ("x+", "z+") if sign == 1 else ("x-", "z-")
        half_a = (a0, a1) if sign == 1 else (a1, a2)
        half_b = (a2, b1) if sign == 1 else (b1, b2)
        copies[x_link, n, "A", 0] = ((), (a0, a2), (0, 0))
        copies[x_link, n, "A", 1] = (((x_link, n, "A", 0),), half_a, (-sign, 0))
        for o in (0, -1, 1, -2, 2, -3, 3, 4):
            if o == 0:
                wanted = ()
            elif o == 4:
                wanted = (("z+", n, "B", 3), ("z-", n, "B", 3))
            else:
                wanted = (("z+" if o < 0 else "z-", n, "B", abs(o) - 1),)
            copies[x_link, n, "B", o] = (wanted, (a2, b2), (0, o))
            copies[x_link, n, "C", o] = (((x_link, n, "B", o),), half_b, (-sign, o))
        for hop in range(4):
            wanted = ((z_link, n, "B", hop - 1),) if hop else ()
            copies[z_link, n, "B", hop] = (wanted, half_b if hop == 3 else (a2, b2), (0, -sign * hop))
        for i in (0, -1, 1, 2):
            ends = (("x+", n, "A", 1), ("x-", n, "A", 1))
            first = {0: (), -1: (("x+", n, "A", 0),), 1: (("x-", n, "A", 0),), 2: ends}[i]
            for hop in range(4):
                wanted = ((z_link, n, "A", hop - 1, i),) if hop else first
                copies[z_link, n, "A", hop, i] = (wanted, half_a if hop == 3 else (a0, a2), (i, -sign * hop))
    return copies


def in_order(copies, ready_at, rate=46.6e3, latency=2.5, queue=2):
    length = {key: size / rate for key, (_, size) in copies.items()}
    after = {key: [] for key in copies}
    for key, (wanted, _) in copies.items():
        for other in wanted:
            after[other].append(key)
    chain = {}

    def chain_of(key):
        if key not in chain:
            chain[key] = length[key] + max([chain_of(k) for k in after[key]], default=0.0)
        return chain[key]

    left, ready, queued = list(copies), {link: [] for link in LINKS}, {link: [] for link in LINKS}
    free = {link: 0.0 for link in LINKS}
    arrival, start, now = {}, {}, 0.0
    while left or any(ready.values()):
        for key in list(left):
            if ready_at(key) <= now + 1e-9 and all(k in arrival and arrival[k] <= now + 1e-9 for k in copies[key][0]):
                left.remove(key)
                ready[key[0]].append(key)
        for link in LINKS:
            queued[link] = [t for t in queued[link] if t > now + 1e-9]
            while ready[link] and len(queued[link]) < queue:
                key = max(ready[link], key=lambda k: (-k[1], chain_of(k)))
                ready[link].remove(key)
                start[key] = now
                free[link] = max(now, free[link]) + length[key]
                queued[link].append(free[link])
                arrival[key] = free[link] + latency
        times = [t for t in arrival.values() if t > now + 1e-9] + [t for q in queued.values() for t in q if t > now + 1e-9]
        times += [ready_at(key) for key in left if ready_at(key) > now + 1e-9]
        now = min(times, default=now)
    return start, arrival


def seen_from_receiver(key, at):
    dx, dz = STEP[key[0]]
    return (at[0] - dx) % X, (at[1] - dz) % Z


GATHER = plan(GATHER_CUTS)
KEYS = list(GATHER)
NUMBER = {key: n for n, key in enumerate(KEYS)}


def kernel(
    arriving_hbm, gain_hbm, w_query, w_key, w_value, w_out,
    sums, entering,
    arriving, gain, hidden, wq, wkv_raw, wkv, wo, stage, acc, squares, cos_q, sin_q, turn_kv, q_rot, own_kv, column_kv, all_kv, keys, values,
    own_context, context, term, landed, whole, leaving, final,
    block_sem, w_sem, wo_sem, shift_send, shift_recv, gather_send, gather_recv, weight_send, weight_recv, x_send, x_recv, z_send, z_recv,
    context_send, context_recv, scatter_send, scatter_recv, final_send, final_recv,
):
    me = lax.axis_index("mp")
    section = lax.axis_index("section")
    x, z = me // Z, lax.rem(me, Z)

    def near(dx, dz):
        return lax.rem(x + dx % X, X) * Z + lax.rem(z + dz % Z, Z)

    loads = [
        pltpu.make_async_copy(w_key.at[0], wkv_raw.at[0], w_sem.at[0]),
        pltpu.make_async_copy(w_value.at[0], wkv_raw.at[1], w_sem.at[1]),
        pltpu.make_async_copy(w_query.at[0], wq, w_sem.at[2]),
    ]

    def out_weights(place, tile):
        return w_out.at[0, :, pl.ds(pl.multiple_of(place * (D // X) + tile * TILE, TILE), TILE)]

    def from_place(place):
        return pl.ds(pl.multiple_of(place * WIDTH, WIDTH), WIDTH)

    for tile in range(TILES):
        loads.append(pltpu.make_async_copy(out_weights(x, tile), wo.at[tile, from_place(x)], wo_sem.at[tile]))
    block_load = pltpu.make_async_copy(arriving_hbm, arriving, block_sem.at[0])
    gain_load = pltpu.make_async_copy(gain_hbm, gain, block_sem.at[1])
    block_load.start()
    gain_load.start()
    for load in loads:
        load.start()

    barrier = pltpu.get_barrier_semaphore()
    for step in range(1, X):
        pl.semaphore_signal(barrier, inc=1, device_id={"mp": near(step, 0)}, device_id_type=MESH)
    for step in range(1, Z):
        pl.semaphore_signal(barrier, inc=1, device_id={"mp": near(0, step)}, device_id_type=MESH)
    for step in (1, SECTIONS - 1):
        pl.semaphore_signal(
            barrier, inc=1, device_id={"section": lax.rem(section + step, SECTIONS)}, device_id_type=MESH
        )
    pl.semaphore_wait(barrier, (X - 1) + (Z - 1) + 2)

    block_load.wait()
    parts = (GATHER_CUTS[0:3:2], GATHER_CUTS[2:5:2])
    shifts = []
    for s, (low, high) in enumerate(parts):
        rows = pl.ds(low, high - low)
        shifts.append(
            pltpu.make_async_remote_copy(
                src_ref=arriving.at[0, rows],
                dst_ref=hidden.at[me, rows],
                send_sem=shift_send.at[s],
                recv_sem=shift_recv.at[s],
                device_id={"section": lax.rem(section + 1, SECTIONS)},
                device_id_type=MESH,
            )
        )
        shifts[-1].start()

    gain_load.wait()
    loads[0].wait()
    loads[1].wait()
    out_row = lax.broadcasted_iota(jnp.int32, (128, 64), 0)
    raw_row = lax.broadcasted_iota(jnp.int32, (128, 64), 1)
    head, j = lax.rem(out_row, 64) // 8, lax.rem(out_row, 8)
    channel = lax.rem(j, 4)
    turned = jnp.where(out_row >= 64, channel + 1 - 2 * lax.rem(channel, 2), channel)
    source = (j // 4) * 32 + (turned // 2) * 16 + head * 2 + lax.rem(turned, 2)
    pick = (raw_row == source).astype(F32).astype(BF16)
    for part in range(8):
        columns = pl.ds(part * (D // 8), D // 8)
        raw = jnp.concatenate([wkv_raw[0, :, columns], wkv_raw[1, :, columns]], axis=0)
        wkv[:, columns] = jnp.dot(pick, raw, preferred_element_type=F32).astype(BF16)

    def passed(key):
        _, (low, high), at = GATHER[key]
        block = hidden.at[near(*at), pl.ds(low, high - low)]
        return pltpu.make_async_remote_copy(
            src_ref=block,
            dst_ref=block,
            send_sem=gather_send.at[NUMBER[key]],
            recv_sem=gather_recv.at[NUMBER[key]],
            device_id={"mp": near(*STEP[key[0]])},
            device_id_type=MESH,
        )

    def weights(key):
        link, _, kind, i = key
        way = STEP[link][0]
        side = 0 if way == 1 else 1
        slot = {"W": 0, "V": TILES, "U": TILES + TILES // 2}[kind] + i
        if kind == "W":
            source, target = out_weights(lax.rem(x + way + X, X), i), wo.at[i, from_place(x)]
        elif kind == "V":
            source, target = out_weights(lax.rem(x + 2, X), FAR_TILES[link][i]), stage.at[side, i]
        else:
            source, target = stage.at[side, i], wo.at[FAR_TILES[link][i], from_place(lax.rem(x - way + X, X))]
        return pltpu.make_async_remote_copy(
            src_ref=source,
            dst_ref=target,
            send_sem=weight_send.at[side, slot],
            recv_sem=weight_recv.at[side, slot],
            device_id={"mp": near(way, 0)},
            device_id_type=MESH,
        )

    def arrived_block(key):
        _, (low, high), at = GATHER[key]
        block = hidden.at[near(*seen_from_receiver(key, at)), pl.ds(low, high - low)]
        return pltpu.make_async_remote_copy(
            src_ref=block,
            dst_ref=block,
            send_sem=gather_send.at[NUMBER[key]],
            recv_sem=gather_recv.at[NUMBER[key]],
            device_id={"mp": near(*STEP[key[0]])},
            device_id_type=MESH,
        )

    started_rows = set()

    def project(part, at):
        owner = near(*at)
        rows = pl.ds(parts[part][0], parts[part][1] - parts[part][0])
        columns = pl.ds(pl.multiple_of(owner * WIDTH, WIDTH), WIDTH)
        block = hidden[owner, rows].astype(F32)
        squared = block * block
        squared = squared[:, :128] + squared[:, 128:]
        scaled = (block * gain[:, columns].astype(F32)).astype(BF16)
        contract = (((1,), (1,)), ((), ()))
        queries = lax.dot_general(scaled, wq[:, columns], contract, preferred_element_type=F32)
        others = lax.dot_general(scaled, wkv[:, columns], contract, preferred_element_type=F32)
        if part not in started_rows:
            started_rows.add(part)
            squares[rows] = squared
            acc[rows, :WIDTH] = queries
            acc[rows, WIDTH:] = others
        else:
            squares[rows] += squared
            acc[rows, :WIDTH] += queries
            acc[rows, WIDTH:] += others

    def rotary_table(i):
        size = 64
        rows = pl.ds(i * size, size)
        lane = lax.broadcasted_iota(jnp.int32, (size, HD), 1)
        token = (lax.broadcasted_iota(jnp.int32, (size, HD), 0) + i * size).astype(F32)
        sign = jnp.where(lax.rem(lane, 2) == 0, -1.0, 1.0)

        def angle(pair):
            return token * jnp.exp(pair.astype(F32) * (-2.0 * math.log(ROPE_BASE) / HD))

        turn = angle(lane // 2)
        cos_q[rows] = jnp.cos(turn)
        sin_q[rows] = jnp.sin(turn) * sign
        j = lax.rem(lane, 8)
        turn = angle(2 * me + lax.rem(j, 4) // 2)
        stay = jnp.where(j < 4, jnp.cos(turn), 1.0)
        cross = jnp.where(j < 4, jnp.sin(turn) * sign, 0.0)
        turn_kv[rows] = jnp.where(lane < 64, stay, cross)

    def scale_of(rows):
        mean = jnp.sum(squares[rows], axis=1, keepdims=True) * (1.0 / D)
        return lax.rsqrt(mean + EPS)

    blocks = ((0,), (1,), (2,))
    x_copies, z_copies = {}, {}

    def send_along_x(n):
        for t in blocks[n]:
            rows = pl.ds(t * QB, QB)
            both = acc[rows, WIDTH:] * scale_of(rows) * turn_kv[rows]
            ready = (both + pltpu.roll(both, 64, 1)).T
            for h in range(KV_HEADS):
                tile = ready[8 * h : 8 * h + 8]
                own_kv[h, t] = jnp.concatenate([tile[:, :128], tile[:, 128:]], axis=0).astype(BF16)
        these = pl.ds(blocks[n][0], len(blocks[n]))
        for step in (2, 1, 3):
            to = lax.rem(x + step, X)
            copy = pltpu.make_async_remote_copy(
                src_ref=own_kv.at[pl.ds(2 * to, 2), these],
                dst_ref=column_kv.at[x, :, these],
                send_sem=x_send.at[n, step - 1],
                recv_sem=x_recv.at[n, step - 1],
                device_id={"mp": near(step, 0)},
                device_id_type=MESH,
            )
            copy.start()
            x_copies[n, step] = copy
        for h in range(2):
            column_kv[x, h, these] = own_kv[2 * x + h, these]

    def send_along_z(n):
        these = pl.ds(blocks[n][0], len(blocks[n]))
        for step in range(1, X):
            x_copies[n, step].wait_recv()
        for step in (4, 3, 5, 2, 6, 1, 7):
            to = lax.rem(z + step, Z)
            copy = pltpu.make_async_remote_copy(
                src_ref=column_kv.at[:, to // 4, these],
                dst_ref=all_kv.at[:, z, these],
                send_sem=z_send.at[n, step - 1],
                recv_sem=z_recv.at[n, step - 1],
                device_id={"mp": near(0, step)},
                device_id_type=MESH,
            )
            copy.start()
            z_copies[n, step] = copy
        for t in blocks[n]:
            all_kv[:, z, t] = column_kv[:, z // 4, t]

    def turn_queries(t):
        lane = lax.broadcasted_iota(jnp.int32, (QB, HD), 1)
        even = lax.rem(lane, 2) == 0
        rows = pl.ds(t * QB, QB)
        scale = scale_of(rows)
        for h in range(2):
            query = acc[rows, h * HD : (h + 1) * HD] * scale
            swapped = jnp.where(even, pltpu.roll(query, HD - 1, 1), pltpu.roll(query, 1, 1))
            rotated = query * cos_q[rows] + swapped * sin_q[rows]
            q_rot[rows, h * HD : (h + 1) * HD] = rotated.astype(BF16)

    def sort_keys(n):
        for step in range(1, Z):
            z_copies[n, step].wait_recv()
        want = lax.broadcasted_iota(jnp.int32, (512, 512), 0)
        have = lax.broadcasted_iota(jnp.int32, (512, 512), 1)
        channel = lax.rem(want, 128)
        source = 16 * (channel // 4) + 4 * (want // 128) + lax.rem(channel, 4)
        pick = (have == source).astype(F32).astype(BF16)
        for t in blocks[n]:
            arrived = all_kv[:, :, t].reshape(512, 128)
            sorted_rows = jnp.dot(pick, arrived, preferred_element_type=F32).astype(BF16)
            for half in range(2):
                columns = slice(t * QB + half * 128, t * QB + half * 128 + 128)
                keys[:, columns] = sorted_rows[256 * half : 256 * half + 128]
                values[:, columns] = sorted_rows[256 * half + 128 : 256 * half + 256]

    def attend(t, h):
        rows = slice(t * SPAN, (t + 1) * SPAN)
        reach = -(-(t + 1) * SPAN // 128) * 128
        token = lax.broadcasted_iota(jnp.int32, (SPAN, reach), 0) + t * SPAN
        causal = token >= lax.broadcasted_iota(jnp.int32, (SPAN, reach), 1)
        scores = jnp.dot(
            q_rot[rows, h * HD : (h + 1) * HD], keys[:, :reach], preferred_element_type=F32
        ) * (1.0 / math.sqrt(HD))
        scores = jnp.where(causal, scores, -1e30)
        exponent = jnp.exp(scores - jnp.max(scores, axis=1, keepdims=True))
        probs = (exponent / jnp.sum(exponent, axis=1, keepdims=True)).astype(BF16)
        mixed = lax.dot_general(
            probs, values[:, :reach], (((1,), (1,)), ((), ())), preferred_element_type=F32
        )
        for place in range(Z):
            own_context[place, t * ROWS : (t + 1) * ROWS, h * HD : (h + 1) * HD] = mixed[place * ROWS : (place + 1) * ROWS]

    own_part = {("A", 0): 0, ("B", 0): 1, ("A", 0, 0): 0}
    own_at = (4.5, 7.0)
    copies = {key: (wanted, (rows[1] - rows[0]) * 2 * WIDTH) for key, (wanted, rows, _) in GATHER.items()}
    for link in ("x+", "x-"):
        for i in range(EARLY_FAR):
            copies[link, 1, "V", i] = ((), WIDTH * TILE * 2)
            copies[link, 1, "U", i] = (((link, 1, "V", i),), WIDTH * TILE * 2)

    def own_ready(key):
        return 0.0 if key[1] or GATHER[key][0] else own_at[own_part[key[2:]]]

    start, arrival = in_order(copies, own_ready)
    bringing = {((0, 0), part): [] for part in range(len(parts))}
    for key, (_, (low, _), at) in GATHER.items():
        part = int(low >= parts[1][0])
        bringing.setdefault((seen_from_receiver(key, at), part), []).append(key)
    events = [(t, 0, "weights" if key[1] else "pass", key) for key, t in start.items()]
    events += [
        (max([arrival[k] + 1.0 for k in by], default=own_at[which[1]] + 0.1), 1, "project", which)
        for which, by in bringing.items()
    ]
    events += [(5.0 + 1.5 * i, 2, "table", i) for i in range(12)]
    events.sort(key=lambda event: event[:2])
    waited = set()

    def need(key):
        if key not in waited:
            waited.add(key)
            (weights if key[1] else arrived_block)(key).wait_recv()

    def need_own(part):
        if ("own", part) not in waited:
            waited.add(("own", part))
            shifts[part].wait_recv()

    query_weights_here = False
    for _, _, what, which in events:
        if what == "pass":
            for key in GATHER[which][0]:
                need(key)
            if not GATHER[which][0]:
                need_own(own_part[which[2:]])
            passed(which).start()
        elif what == "project":
            if not query_weights_here:
                query_weights_here = True
                loads[2].wait()
            for key in bringing[which]:
                need(key)
            if not bringing[which]:
                need_own(which[1])
            project(which[1], which[0])
        elif what == "weights":
            for key in copies[which][0]:
                need(key)
            weights(which).start()
        else:
            rotary_table(which)

    for t in range(3):
        send_along_x(t)
    for t in range(3):
        turn_queries(t)
    for t in range(3):
        send_along_z(t)
    for i in range(TILES // 2):
        for link in ("x+", "x-"):
            weights((link, 1, "W", i)).start()
    for i in range(EARLY_FAR, TILES // 2):
        for link in ("x+", "x-"):
            weights((link, 1, "V", i)).start()
    for key in KEYS:
        passed(key).wait_send()
    for shift in shifts:
        shift.wait_send()
    first = me * ROWS
    offset = lax.rem(me, 2) * 8
    window = pl.ds(pl.multiple_of(first - offset, 16), ROWS + 8)
    for unit in range(N):
        wide = hidden[unit, window].astype(F32)
        residual = jnp.where(offset == 0, wide[:ROWS], wide[8:])
        entering[0, :, unit * WIDTH : (unit + 1) * WIDTH] = residual.astype(BF16)
    for t in range(X):
        if t < 3:
            sort_keys(t)
        for h in range(2):
            attend(t, h)
    for place in range(Z):
        context[x, place] = own_context[place].astype(BF16)
    for copy in list(x_copies.values()) + list(z_copies.values()):
        copy.wait_send()

    def hand_context(link, hop, i):
        way = STEP[link][0]
        side = 0 if way == 1 else 1
        place = lax.rem(z + NEAREST_LAST[i] + Z, Z)
        if hop == 0:
            part = context.at[x, place]
        else:
            part = context.at[lax.rem(x - way + X, X), place, pl.ds(side * (BAND // 2), BAND // 2)]
        return pltpu.make_async_remote_copy(
            src_ref=part,
            dst_ref=part,
            send_sem=context_send.at[side, hop, i],
            recv_sem=context_recv.at[side, hop, i],
            device_id={"mp": near(way, 0)},
            device_id_type=MESH,
        )

    def place_of(i):
        return lax.rem(z + NEAREST_LAST[i] + Z, Z)

    made = set()

    def make_terms(i, tile):
        if (i, tile) in made:
            return
        these = [n for n, away in enumerate(NEAREST_LAST) if abs(away) == abs(NEAREST_LAST[i])]
        made.update((n, tile) for n in these)
        for n in these:
            for link in ("x+", "x-"):
                need_late((link, "Q", n))
        if tile not in made:
            made.add(tile)
            loads[3 + tile].wait()
            for link in ("x+", "x-"):
                need_late((link, "W", tile))
                if tile in FAR_TILES[link]:
                    need_late((link, "U", FAR_TILES[link].index(tile)))
        mixed = [jnp.concatenate([context[c, place_of(n)] for c in range(X)], axis=1) for n in these]
        product = jnp.dot(jnp.concatenate(mixed, axis=0), wo[tile], preferred_element_type=F32).astype(BF16)
        for m, n in enumerate(these):
            term[n, tile] = product[m * BAND : (m + 1) * BAND]

    def handed(way, step, tile):
        side = 0 if way == 1 else 1
        return pltpu.make_async_remote_copy(
            src_ref=term.at[NEAREST_LAST.index(way * (4 - step) if step else 4), tile],
            dst_ref=landed.at[side, step, tile],
            send_sem=scatter_send.at[side, step, tile],
            recv_sem=scatter_recv.at[side, step, tile],
            device_id={"mp": near(0, way)},
            device_id_type=MESH,
        )

    def starts_here(way, step, tile):
        return step == 0 or (step == 1 and tile % 2 != (0 if way == 1 else 1))

    def hand_on(way, step, tile):
        if not starts_here(way, step, tile):
            handed(way, step - 1, tile).wait_recv()
            i = NEAREST_LAST.index(way * (4 - step))
            total = term[i, tile].astype(F32) + landed[0 if way == 1 else 1, step - 1, tile].astype(F32)
            term[i, tile] = total.astype(BF16)
        handed(way, step, tile).start()

    def leave(pair, step):
        to = lax.rem(x + step, X)
        return pltpu.make_async_remote_copy(
            src_ref=leaving.at[to, pair],
            dst_ref=final.at[x, pair],
            send_sem=final_send.at[step - 1, pair],
            recv_sem=final_recv.at[step - 1, pair],
            device_id={"mp": near(step, 0)},
            device_id_type=MESH,
        )

    def finish(pair):
        for tile in (2 * pair, 2 * pair + 1):
            make_terms(NEAREST_LAST.index(0), tile)
            total = term[NEAREST_LAST.index(0), tile].astype(F32)
            for way in (1, -1):
                handed(way, 3, tile).wait_recv()
                total += landed[0 if way == 1 else 1, 3, tile].astype(F32)
            whole[tile % 2] = total
        for to in range(X):
            rows = slice(to * ROWS, (to + 1) * ROWS)
            leaving[to, pair] = jnp.concatenate([whole[0, rows], whole[1, rows]], axis=0).astype(BF16)
        for step in range(1, X):
            leave(pair, step).start()
        final[x, pair] = leaving[x, pair]

    def write(pair):
        for step in range(1, X):
            leave(pair, step).wait_recv()
        for place in range(X):
            total = final[place, pair]
            at = place * (D // X) + pair * 2 * TILE
            sums[0, :, at : at + TILE] = total[:ROWS]
            sums[0, :, at + TILE : at + 2 * TILE] = total[ROWS:]

    late = {}
    late_tiles = {}
    for link in ("x+", "x-"):
        for i in range(Z):
            late[link, 0, "P", i] = ((), BAND * WIDTH * 2)
            late[link, 0, "Q", i] = (((link, 0, "P", i),), BAND * WIDTH)
        for tile in range(TILES // 2, TILES):
            key = (link, tile // 2 - 1, "W", tile)
            late[key] = ((), WIDTH * TILE * 2)
            late_tiles.setdefault(tile, []).append(key)
        for i in range(EARLY_FAR, TILES // 2):
            tile = FAR_TILES[link][i]
            key = (link, tile // 2 - 1, "U", i)
            late[key] = ((), WIDTH * TILE * 2)
            late_tiles.setdefault(tile, []).append(key)
    for way, link in ((1, "z+"), (-1, "z-")):
        for tile in range(TILES):
            rank = max(tile // 2 - 1, 0)
            for step in range(4):
                if step == 0 and starts_here(way, 1, tile):
                    continue
                away = way * (4 - step) if step else 4
                wanted = [(l, 0, "Q", n) for l in ("x+", "x-") for n, a in enumerate(NEAREST_LAST) if abs(a) == abs(away)]
                wanted += late_tiles.get(tile, [])
                if not starts_here(way, step, tile):
                    wanted.append((link, rank, "S", tile, step - 1))
                late[link, rank, "S", tile, step] = (tuple(wanted), BAND * TILE * 2)
    start, arrival = in_order(late, lambda key: 0.0)
    here = set()

    def need_late(key):
        if key not in here:
            here.add(key)
            link, kind, i = key
            if kind in "PQ":
                hand_context(link, 0 if kind == "P" else 1, i).wait_recv()
            else:
                need((link, 1, kind, i))

    events = [(t, 0, "copy", key) for key, t in start.items()]
    for pair in range(PAIRS):
        tiles = (2 * pair, 2 * pair + 1)
        there = max(arrival[link, max(pair - 1, 0), "S", tile, 3] for link in ("z+", "z-") for tile in tiles)
        events += [(there + 0.5, 1, "finish", pair), (there + 6.5, 2, "write", pair)]
    events.sort(key=lambda event: event[:2])
    for _, _, what, which in events:
        if what == "finish":
            finish(which)
        elif what == "write":
            write(which)
        elif which[2] == "P":
            hand_context(which[0], 0, which[3]).start()
        elif which[2] == "Q":
            need_late((which[0], "P", which[3]))
            hand_context(which[0], 1, which[3]).start()
        elif which[2] in "WU":
            if which[2] == "U":
                need((which[0], 1, "V", which[3]))
            weights((which[0], 1, which[2], which[3])).start()
        else:
            link, _, _, tile, step = which
            way = 1 if link == "z+" else -1
            make_terms(NEAREST_LAST.index(way * (4 - step) if step else 4), tile)
            hand_on(way, step, tile)

    for link in ("x+", "x-"):
        for i in range(TILES):
            weights((link, 1, "W", i)).wait_send()
        for i in range(TILES // 2):
            weights((link, 1, "V", i)).wait_send()
            weights((link, 1, "U", i)).wait_send()
        for i in range(Z):
            for hop in range(2):
                hand_context(link, hop, i).wait_send()
    for way in (1, -1):
        for tile in range(TILES):
            for step in range(4):
                if step or tile % 2 == (0 if way == 1 else 1):
                    handed(way, step, tile).wait_send()
    for pair in range(PAIRS):
        for step in range(1, X):
            leave(pair, step).wait_send()


def finish_kernel(summed, entering, attended, stream):
    attended[...] = summed[...]
    stream[...] = (entering[...].astype(F32) + summed[...].astype(F32)).astype(BF16)


def layer(arriving, norm_gain, w_query, w_key, w_value, w_out):
    any_space = pl.BlockSpec(memory_space=pl.ANY)
    vmem = pl.BlockSpec(memory_space=pltpu.VMEM)
    out = jax.ShapeDtypeStruct((1, ROWS, D), BF16)
    dma = pltpu.SemaphoreType.DMA
    summed, residual = pl.pallas_call(
        kernel,
        out_shape=(out, out),
        in_specs=[any_space, any_space, any_space, any_space, any_space, any_space],
        out_specs=(vmem, vmem),
        scratch_shapes=[
            pltpu.VMEM((1, LENGTH, WIDTH), BF16),
            pltpu.VMEM((1, D), BF16),
            pltpu.VMEM((N, LENGTH, WIDTH), BF16),
            pltpu.VMEM((WIDTH, D), BF16),
            pltpu.VMEM((2, 32, D), BF16),
            pltpu.VMEM((128, D), BF16),
            pltpu.VMEM((TILES, X * WIDTH, TILE), BF16),
            pltpu.VMEM((2, TILES // 2, WIDTH, TILE), BF16),
            pltpu.VMEM((LENGTH, WIDTH + 128), F32),
            pltpu.VMEM((LENGTH, 128), F32),
            pltpu.VMEM((LENGTH, HD), F32),
            pltpu.VMEM((LENGTH, HD), F32),
            pltpu.VMEM((LENGTH, HD), F32),
            pltpu.VMEM((LENGTH, WIDTH), BF16),
            pltpu.VMEM((KV_HEADS, 3, 16, 128), BF16),
            pltpu.VMEM((X, 2, 3, 16, 128), BF16),
            pltpu.VMEM((X, Z, 3, 16, 128), BF16),
            pltpu.VMEM((HD, LENGTH), BF16),
            pltpu.VMEM((HD, LENGTH), BF16),
            pltpu.VMEM((Z, BAND, WIDTH), F32),
            pltpu.VMEM((X, Z, BAND, WIDTH), BF16),
            pltpu.VMEM((Z, TILES, BAND, TILE), BF16),
            pltpu.VMEM((2, 4, TILES, BAND, TILE), BF16),
            pltpu.VMEM((2, BAND, TILE), F32),
            pltpu.VMEM((X, PAIRS, 2 * ROWS, TILE), BF16),
            pltpu.VMEM((X, PAIRS, 2 * ROWS, TILE), BF16),
            dma((2,)),
            dma((3,)),
            dma((TILES,)),
            dma((2,)),
            dma((2,)),
            dma((len(KEYS),)),
            dma((len(KEYS),)),
            dma((2, 2 * TILES)),
            dma((2, 2 * TILES)),
            dma((3, X - 1)),
            dma((3, X - 1)),
            dma((3, Z - 1)),
            dma((3, Z - 1)),
            dma((2, 2, Z)),
            dma((2, 2, Z)),
            dma((2, 4, TILES)),
            dma((2, 4, TILES)),
            dma((X - 1, PAIRS)),
            dma((X - 1, PAIRS)),
        ],
        compiler_params=pltpu.CompilerParams(
            collective_id=0, has_side_effects=True, vmem_limit_bytes=67043328
        ),
    )(arriving, norm_gain, w_query, w_key, w_value, w_out)
    return pl.pallas_call(finish_kernel, out_shape=(out, out), in_specs=[vmem, vmem], out_specs=(vmem, vmem))(summed, residual)


def solution(mesh):
    return jax.shard_map(
        layer,
        mesh=mesh,
        in_specs=(
            P("section", None, "mp"),
            P("section", None),
            P("section", "mp", None),
            P("section", "mp", None),
            P("section", "mp", None),
            P("section", "mp", None),
        ),
        out_specs=(P("section", "mp", None), P("section", "mp", None)),
        check_vma=False,
    )
```

```python
import math

import jax
import jax.numpy as jnp
from jax import lax
from jax.experimental import pallas as pl
from jax.experimental.pallas import tpu as pltpu
from jax.sharding import PartitionSpec as P

MESH = pl.DeviceIdType.MESH
BF16 = jnp.bfloat16
F32 = jnp.float32

X = 4
Z = 8
N = X * Z
SECTIONS = 8
LENGTH = 768
D = 8192
HD = 128
KV_HEADS = 8
WIDTH = D // N
ROWS = LENGTH // N
QB = 256
SPAN = ROWS * Z
TILE = 256
TILES = D // X // TILE
PAIRS = TILES // 2
BAND = X * ROWS

ROPE_BASE = 500000.0
EPS = 1e-05

LINKS = ("x+", "x-", "z+", "z-")
STEP = {"x+": (1, 0), "x-": (-1, 0), "z+": (0, 1), "z-": (0, -1)}
GATHER_CUTS = (0, 192, 384, 576, 768)
FAR_TILES = {"x+": (0, 2, 4, 6), "x-": (1, 3, 5, 7)}
EARLY_FAR = 4
NEAREST_LAST = (4, 3, -3, 2, -2, 1, -1, 0)


def plan(cuts):
    copies = {}
    n = 0
    a0, a1, a2, b1, b2 = cuts
    for sign in (1, -1):
        x_link, z_link = ("x+", "z+") if sign == 1 else ("x-", "z-")
        half_a = (a0, a1) if sign == 1 else (a1, a2)
        half_b = (a2, b1) if sign == 1 else (b1, b2)
        copies[x_link, n, "A", 0] = ((), (a0, a2), (0, 0))
        copies[x_link, n, "A", 1] = (((x_link, n, "A", 0),), half_a, (-sign, 0))
        for o in (0, -1, 1, -2, 2, -3, 3, 4):
            if o == 0:
                wanted = ()
            elif o == 4:
                wanted = (("z+", n, "B", 3), ("z-", n, "B", 3))
            else:
                wanted = (("z+" if o < 0 else "z-", n, "B", abs(o) - 1),)
            copies[x_link, n, "B", o] = (wanted, (a2, b2), (0, o))
            copies[x_link, n, "C", o] = (((x_link, n, "B", o),), half_b, (-sign, o))
        for hop in range(4):
            wanted = ((z_link, n, "B", hop - 1),) if hop else ()
            copies[z_link, n, "B", hop] = (wanted, half_b if hop == 3 else (a2, b2), (0, -sign * hop))
        for i in (0, -1, 1, 2):
            ends = (("x+", n, "A", 1), ("x-", n, "A", 1))
            first = {0: (), -1: (("x+", n, "A", 0),), 1: (("x-", n, "A", 0),), 2: ends}[i]
            for hop in range(4):
                wanted = ((z_link, n, "A", hop - 1, i),) if hop else first
                copies[z_link, n, "A", hop, i] = (wanted, half_a if hop == 3 else (a0, a2), (i, -sign * hop))
    return copies


def in_order(copies, ready_at, rate=46.6e3, latency=2.5, queue=2):
    length = {key: size / rate for key, (_, size) in copies.items()}
    after = {key: [] for key in copies}
    for key, (wanted, _) in copies.items():
        for other in wanted:
            after[other].append(key)
    chain = {}

    def chain_of(key):
        if key not in chain:
            chain[key] = length[key] + max([chain_of(k) for k in after[key]], default=0.0)
        return chain[key]

    left, ready, queued = list(copies), {link: [] for link in LINKS}, {link: [] for link in LINKS}
    free = {link: 0.0 for link in LINKS}
    arrival, start, now = {}, {}, 0.0
    while left or any(ready.values()):
        for key in list(left):
            if ready_at(key) <= now + 1e-9 and all(k in arrival and arrival[k] <= now + 1e-9 for k in copies[key][0]):
                left.remove(key)
                ready[key[0]].append(key)
        for link in LINKS:
            queued[link] = [t for t in queued[link] if t > now + 1e-9]
            while ready[link] and len(queued[link]) < queue:
                key = max(ready[link], key=lambda k: (-k[1], chain_of(k)))
                ready[link].remove(key)
                start[key] = now
                free[link] = max(now, free[link]) + length[key]
                queued[link].append(free[link])
                arrival[key] = free[link] + latency
        times = [t for t in arrival.values() if t > now + 1e-9] + [t for q in queued.values() for t in q if t > now + 1e-9]
        times += [ready_at(key) for key in left if ready_at(key) > now + 1e-9]
        now = min(times, default=now)
    return start, arrival


def seen_from_receiver(key, at):
    dx, dz = STEP[key[0]]
    return (at[0] - dx) % X, (at[1] - dz) % Z


GATHER = plan(GATHER_CUTS)
KEYS = list(GATHER)
NUMBER = {key: n for n, key in enumerate(KEYS)}


def kernel(
    arriving_hbm, gain_hbm, w_query, w_key, w_value, w_out,
    sums, entering,
    arriving, gain, hidden, wq, wkv_raw, wkv, wo, stage, acc, squares, cos_q, sin_q, turn_kv, q_rot, own_kv, column_kv, all_kv, keys, values,
    own_context, context, term, landed, whole, leaving, final,
    block_sem, w_sem, wo_sem, shift_send, shift_recv, gather_send, gather_recv, weight_send, weight_recv, x_send, x_recv, z_send, z_recv,
    context_send, context_recv, scatter_send, scatter_recv, final_send, final_recv,
):
    me = lax.axis_index("mp")
    section = lax.axis_index("section")
    x, z = me // Z, lax.rem(me, Z)

    def near(dx, dz):
        return lax.rem(x + dx % X, X) * Z + lax.rem(z + dz % Z, Z)

    loads = [
        pltpu.make_async_copy(w_key.at[0], wkv_raw.at[0], w_sem.at[0]),
        pltpu.make_async_copy(w_value.at[0], wkv_raw.at[1], w_sem.at[1]),
        pltpu.make_async_copy(w_query.at[0], wq, w_sem.at[2]),
    ]

    def out_weights(place, tile):
        return w_out.at[0, :, pl.ds(pl.multiple_of(place * (D // X) + tile * TILE, TILE), TILE)]

    def from_place(place):
        return pl.ds(pl.multiple_of(place * WIDTH, WIDTH), WIDTH)

    for tile in range(TILES):
        loads.append(pltpu.make_async_copy(out_weights(x, tile), wo.at[tile, from_place(x)], wo_sem.at[tile]))
    block_load = pltpu.make_async_copy(arriving_hbm, arriving, block_sem.at[0])
    gain_load = pltpu.make_async_copy(gain_hbm, gain, block_sem.at[1])
    block_load.start()
    gain_load.start()
    for load in loads:
        load.start()

    barrier = pltpu.get_barrier_semaphore()
    for step in (1, X - 1):
        pl.semaphore_signal(barrier, inc=1, device_id={"mp": near(step, 0)}, device_id_type=MESH)
    for step in (1, Z - 1):
        pl.semaphore_signal(barrier, inc=1, device_id={"mp": near(0, step)}, device_id_type=MESH)
    for step in (1, SECTIONS - 1):
        pl.semaphore_signal(
            barrier, inc=1, device_id={"section": lax.rem(section + step, SECTIONS)}, device_id_type=MESH
        )
    pl.semaphore_wait(barrier, 6)

    block_load.wait()
    parts = (GATHER_CUTS[0:3:2], GATHER_CUTS[2:5:2])
    shifts = []
    for s, (low, high) in enumerate(parts):
        rows = pl.ds(low, high - low)
        shifts.append(
            pltpu.make_async_remote_copy(
                src_ref=arriving.at[0, rows],
                dst_ref=hidden.at[me, rows],
                send_sem=shift_send.at[s],
                recv_sem=shift_recv.at[s],
                device_id={"section": lax.rem(section + 1, SECTIONS)},
                device_id_type=MESH,
            )
        )
        shifts[-1].start()

    gain_load.wait()
    loads[0].wait()
    loads[1].wait()
    out_row = lax.broadcasted_iota(jnp.int32, (128, 64), 0)
    raw_row = lax.broadcasted_iota(jnp.int32, (128, 64), 1)
    head, j = lax.rem(out_row, 64) // 8, lax.rem(out_row, 8)
    channel = lax.rem(j, 4)
    turned = jnp.where(out_row >= 64, channel + 1 - 2 * lax.rem(channel, 2), channel)
    source = (j // 4) * 32 + (turned // 2) * 16 + head * 2 + lax.rem(turned, 2)
    pick = (raw_row == source).astype(F32).astype(BF16)
    for part in range(8):
        columns = pl.ds(part * (D // 8), D // 8)
        raw = jnp.concatenate([wkv_raw[0, :, columns], wkv_raw[1, :, columns]], axis=0)
        wkv[:, columns] = jnp.dot(pick, raw, preferred_element_type=F32).astype(BF16)

    def passed(key):
        _, (low, high), at = GATHER[key]
        block = hidden.at[near(*at), pl.ds(low, high - low)]
        return pltpu.make_async_remote_copy(
            src_ref=block,
            dst_ref=block,
            send_sem=gather_send.at[NUMBER[key]],
            recv_sem=gather_recv.at[NUMBER[key]],
            device_id={"mp": near(*STEP[key[0]])},
            device_id_type=MESH,
        )

    def weights(key):
        link, _, kind, i = key
        way = STEP[link][0]
        side = 0 if way == 1 else 1
        slot = {"W": 0, "V": TILES, "U": TILES + TILES // 2}[kind] + i
        if kind == "W":
            source, target = out_weights(lax.rem(x + way + X, X), i), wo.at[i, from_place(x)]
        elif kind == "V":
            source, target = out_weights(lax.rem(x + 2, X), FAR_TILES[link][i]), stage.at[side, i]
        else:
            source, target = stage.at[side, i], wo.at[FAR_TILES[link][i], from_place(lax.rem(x - way + X, X))]
        return pltpu.make_async_remote_copy(
            src_ref=source,
            dst_ref=target,
            send_sem=weight_send.at[side, slot],
            recv_sem=weight_recv.at[side, slot],
            device_id={"mp": near(way, 0)},
            device_id_type=MESH,
        )

    def arrived_block(key):
        _, (low, high), at = GATHER[key]
        block = hidden.at[near(*seen_from_receiver(key, at)), pl.ds(low, high - low)]
        return pltpu.make_async_remote_copy(
            src_ref=block,
            dst_ref=block,
            send_sem=gather_send.at[NUMBER[key]],
            recv_sem=gather_recv.at[NUMBER[key]],
            device_id={"mp": near(*STEP[key[0]])},
            device_id_type=MESH,
        )

    started_rows = set()

    def project(part, at):
        owner = near(*at)
        rows = pl.ds(parts[part][0], parts[part][1] - parts[part][0])
        columns = pl.ds(pl.multiple_of(owner * WIDTH, WIDTH), WIDTH)
        block = hidden[owner, rows].astype(F32)
        squared = block * block
        squared = squared[:, :128] + squared[:, 128:]
        scaled = (block * gain[:, columns].astype(F32)).astype(BF16)
        contract = (((1,), (1,)), ((), ()))
        queries = lax.dot_general(scaled, wq[:, columns], contract, preferred_element_type=F32)
        others = lax.dot_general(scaled, wkv[:, columns], contract, preferred_element_type=F32)
        if part not in started_rows:
            started_rows.add(part)
            squares[rows] = squared
            acc[rows, :WIDTH] = queries
            acc[rows, WIDTH:] = others
        else:
            squares[rows] += squared
            acc[rows, :WIDTH] += queries
            acc[rows, WIDTH:] += others

    def rotary_table(i):
        size = 64
        rows = pl.ds(i * size, size)
        lane = lax.broadcasted_iota(jnp.int32, (size, HD), 1)
        token = (lax.broadcasted_iota(jnp.int32, (size, HD), 0) + i * size).astype(F32)
        sign = jnp.where(lax.rem(lane, 2) == 0, -1.0, 1.0)

        def angle(pair):
            return token * jnp.exp(pair.astype(F32) * (-2.0 * math.log(ROPE_BASE) / HD))

        turn = angle(lane // 2)
        cos_q[rows] = jnp.cos(turn)
        sin_q[rows] = jnp.sin(turn) * sign
        j = lax.rem(lane, 8)
        turn = angle(2 * me + lax.rem(j, 4) // 2)
        stay = jnp.where(j < 4, jnp.cos(turn), 1.0)
        cross = jnp.where(j < 4, jnp.sin(turn) * sign, 0.0)
        turn_kv[rows] = jnp.where(lane < 64, stay, cross)

    def scale_of(rows):
        mean = jnp.sum(squares[rows], axis=1, keepdims=True) * (1.0 / D)
        return lax.rsqrt(mean + EPS)

    blocks = ((0,), (1,), (2,))
    x_copies, z_copies = {}, {}

    def send_along_x(n):
        for t in blocks[n]:
            rows = pl.ds(t * QB, QB)
            both = acc[rows, WIDTH:] * scale_of(rows) * turn_kv[rows]
            ready = (both + pltpu.roll(both, 64, 1)).T
            for h in range(KV_HEADS):
                tile = ready[8 * h : 8 * h + 8]
                own_kv[h, t] = jnp.concatenate([tile[:, :128], tile[:, 128:]], axis=0).astype(BF16)
        these = pl.ds(blocks[n][0], len(blocks[n]))
        for step in (2, 1, 3):
            to = lax.rem(x + step, X)
            copy = pltpu.make_async_remote_copy(
                src_ref=own_kv.at[pl.ds(2 * to, 2), these],
                dst_ref=column_kv.at[x, :, these],
                send_sem=x_send.at[n, step - 1],
                recv_sem=x_recv.at[n, step - 1],
                device_id={"mp": near(step, 0)},
                device_id_type=MESH,
            )
            copy.start()
            x_copies[n, step] = copy
        for h in range(2):
            column_kv[x, h, these] = own_kv[2 * x + h, these]

    def send_along_z(n):
        these = pl.ds(blocks[n][0], len(blocks[n]))
        for step in range(1, X):
            x_copies[n, step].wait_recv()
        for step in (4, 3, 5, 2, 6, 1, 7):
            to = lax.rem(z + step, Z)
            copy = pltpu.make_async_remote_copy(
                src_ref=column_kv.at[:, to // 4, these],
                dst_ref=all_kv.at[:, z, these],
                send_sem=z_send.at[n, step - 1],
                recv_sem=z_recv.at[n, step - 1],
                device_id={"mp": near(0, step)},
                device_id_type=MESH,
            )
            copy.start()
            z_copies[n, step] = copy
        for t in blocks[n]:
            all_kv[:, z, t] = column_kv[:, z // 4, t]

    def turn_queries(t):
        lane = lax.broadcasted_iota(jnp.int32, (QB, HD), 1)
        even = lax.rem(lane, 2) == 0
        rows = pl.ds(t * QB, QB)
        scale = scale_of(rows)
        for h in range(2):
            query = acc[rows, h * HD : (h + 1) * HD] * scale
            swapped = jnp.where(even, pltpu.roll(query, HD - 1, 1), pltpu.roll(query, 1, 1))
            rotated = query * cos_q[rows] + swapped * sin_q[rows]
            q_rot[rows, h * HD : (h + 1) * HD] = rotated.astype(BF16)

    def sort_keys(n):
        for step in range(1, Z):
            z_copies[n, step].wait_recv()
        want = lax.broadcasted_iota(jnp.int32, (512, 512), 0)
        have = lax.broadcasted_iota(jnp.int32, (512, 512), 1)
        channel = lax.rem(want, 128)
        source = 16 * (channel // 4) + 4 * (want // 128) + lax.rem(channel, 4)
        pick = (have == source).astype(F32).astype(BF16)
        for t in blocks[n]:
            arrived = all_kv[:, :, t].reshape(512, 128)
            sorted_rows = jnp.dot(pick, arrived, preferred_element_type=F32).astype(BF16)
            for half in range(2):
                columns = slice(t * QB + half * 128, t * QB + half * 128 + 128)
                keys[:, columns] = sorted_rows[256 * half : 256 * half + 128]
                values[:, columns] = sorted_rows[256 * half + 128 : 256 * half + 256]

    def attend(t, h):
        rows = slice(t * SPAN, (t + 1) * SPAN)
        reach = -(-(t + 1) * SPAN // 128) * 128
        token = lax.broadcasted_iota(jnp.int32, (SPAN, reach), 0) + t * SPAN
        causal = token >= lax.broadcasted_iota(jnp.int32, (SPAN, reach), 1)
        scores = jnp.dot(
            q_rot[rows, h * HD : (h + 1) * HD], keys[:, :reach], preferred_element_type=F32
        ) * (1.0 / math.sqrt(HD))
        scores = jnp.where(causal, scores, -1e30)
        exponent = jnp.exp(scores - jnp.max(scores, axis=1, keepdims=True))
        probs = (exponent / jnp.sum(exponent, axis=1, keepdims=True)).astype(BF16)
        mixed = lax.dot_general(
            probs, values[:, :reach], (((1,), (1,)), ((), ())), preferred_element_type=F32
        )
        for place in range(Z):
            own_context[place, t * ROWS : (t + 1) * ROWS, h * HD : (h + 1) * HD] = mixed[place * ROWS : (place + 1) * ROWS]

    own_part = {("A", 0): 0, ("B", 0): 1, ("A", 0, 0): 0}
    own_at = (4.5, 7.0)
    copies = {key: (wanted, (rows[1] - rows[0]) * 2 * WIDTH) for key, (wanted, rows, _) in GATHER.items()}
    for link in ("x+", "x-"):
        for i in range(EARLY_FAR):
            copies[link, 1, "V", i] = ((), WIDTH * TILE * 2)
            copies[link, 1, "U", i] = (((link, 1, "V", i),), WIDTH * TILE * 2)

    def own_ready(key):
        return 0.0 if key[1] or GATHER[key][0] else own_at[own_part[key[2:]]]

    start, arrival = in_order(copies, own_ready)
    bringing = {((0, 0), part): [] for part in range(len(parts))}
    for key, (_, (low, _), at) in GATHER.items():
        part = int(low >= parts[1][0])
        bringing.setdefault((seen_from_receiver(key, at), part), []).append(key)
    events = [(t, 0, "weights" if key[1] else "pass", key) for key, t in start.items()]
    events += [
        (max([arrival[k] + 1.0 for k in by], default=own_at[which[1]] + 0.1), 1, "project", which)
        for which, by in bringing.items()
    ]
    events += [(5.0 + 1.5 * i, 2, "table", i) for i in range(12)]
    events.sort(key=lambda event: event[:2])
    waited = set()

    def need(key):
        if key not in waited:
            waited.add(key)
            (weights if key[1] else arrived_block)(key).wait_recv()

    def need_own(part):
        if ("own", part) not in waited:
            waited.add(("own", part))
            shifts[part].wait_recv()

    query_weights_here = False
    for _, _, what, which in events:
        if what == "pass":
            for key in GATHER[which][0]:
                need(key)
            if not GATHER[which][0]:
                need_own(own_part[which[2:]])
            passed(which).start()
        elif what == "project":
            if not query_weights_here:
                query_weights_here = True
                loads[2].wait()
            for key in bringing[which]:
                need(key)
            if not bringing[which]:
                need_own(which[1])
            project(which[1], which[0])
        elif what == "weights":
            for key in copies[which][0]:
                need(key)
            weights(which).start()
        else:
            rotary_table(which)

    for t in range(3):
        send_along_x(t)
    for t in range(3):
        turn_queries(t)
    for t in range(3):
        send_along_z(t)
    for i in range(TILES // 2):
        for link in ("x+", "x-"):
            weights((link, 1, "W", i)).start()
    for i in range(EARLY_FAR, TILES // 2):
        for link in ("x+", "x-"):
            weights((link, 1, "V", i)).start()
    for key in KEYS:
        passed(key).wait_send()
    for shift in shifts:
        shift.wait_send()
    first = me * ROWS
    offset = lax.rem(me, 2) * 8
    window = pl.ds(pl.multiple_of(first - offset, 16), ROWS + 8)
    for unit in range(N):
        wide = hidden[unit, window].astype(F32)
        residual = jnp.where(offset == 0, wide[:ROWS], wide[8:])
        entering[0, :, unit * WIDTH : (unit + 1) * WIDTH] = residual.astype(BF16)
    for t in range(X):
        if t < 3:
            sort_keys(t)
        for h in range(2):
            attend(t, h)
    for place in range(Z):
        context[x, place] = own_context[place].astype(BF16)
    for copy in list(x_copies.values()) + list(z_copies.values()):
        copy.wait_send()

    def hand_context(link, hop, i):
        way = STEP[link][0]
        side = 0 if way == 1 else 1
        place = lax.rem(z + NEAREST_LAST[i] + Z, Z)
        if hop == 0:
            part = context.at[x, place]
        else:
            part = context.at[lax.rem(x - way + X, X), place, pl.ds(side * (BAND // 2), BAND // 2)]
        return pltpu.make_async_remote_copy(
            src_ref=part,
            dst_ref=part,
            send_sem=context_send.at[side, hop, i],
            recv_sem=context_recv.at[side, hop, i],
            device_id={"mp": near(way, 0)},
            device_id_type=MESH,
        )

    def place_of(i):
        return lax.rem(z + NEAREST_LAST[i] + Z, Z)

    made = set()

    def make_terms(i, tile):
        if (i, tile) in made:
            return
        these = [n for n, away in enumerate(NEAREST_LAST) if abs(away) == abs(NEAREST_LAST[i])]
        made.update((n, tile) for n in these)
        for n in these:
            for link in ("x+", "x-"):
                need_late((link, "Q", n))
        if tile not in made:
            made.add(tile)
            loads[3 + tile].wait()
            for link in ("x+", "x-"):
                need_late((link, "W", tile))
                if tile in FAR_TILES[link]:
                    need_late((link, "U", FAR_TILES[link].index(tile)))
        mixed = [jnp.concatenate([context[c, place_of(n)] for c in range(X)], axis=1) for n in these]
        product = jnp.dot(jnp.concatenate(mixed, axis=0), wo[tile], preferred_element_type=F32).astype(BF16)
        for m, n in enumerate(these):
            term[n, tile] = product[m * BAND : (m + 1) * BAND]

    def handed(way, step, tile):
        side = 0 if way == 1 else 1
        return pltpu.make_async_remote_copy(
            src_ref=term.at[NEAREST_LAST.index(way * (4 - step) if step else 4), tile],
            dst_ref=landed.at[side, step, tile],
            send_sem=scatter_send.at[side, step, tile],
            recv_sem=scatter_recv.at[side, step, tile],
            device_id={"mp": near(0, way)},
            device_id_type=MESH,
        )

    def starts_here(way, step, tile):
        return step == 0 or (step == 1 and tile % 2 != (0 if way == 1 else 1))

    def hand_on(way, step, tile):
        if not starts_here(way, step, tile):
            handed(way, step - 1, tile).wait_recv()
            i = NEAREST_LAST.index(way * (4 - step))
            total = term[i, tile].astype(F32) + landed[0 if way == 1 else 1, step - 1, tile].astype(F32)
            term[i, tile] = total.astype(BF16)
        handed(way, step, tile).start()

    def leave(pair, step):
        to = lax.rem(x + step, X)
        return pltpu.make_async_remote_copy(
            src_ref=leaving.at[to, pair],
            dst_ref=final.at[x, pair],
            send_sem=final_send.at[step - 1, pair],
            recv_sem=final_recv.at[step - 1, pair],
            device_id={"mp": near(step, 0)},
            device_id_type=MESH,
        )

    def finish(pair):
        for tile in (2 * pair, 2 * pair + 1):
            make_terms(NEAREST_LAST.index(0), tile)
            total = term[NEAREST_LAST.index(0), tile].astype(F32)
            for way in (1, -1):
                handed(way, 3, tile).wait_recv()
                total += landed[0 if way == 1 else 1, 3, tile].astype(F32)
            whole[tile % 2] = total
        for to in range(X):
            rows = slice(to * ROWS, (to + 1) * ROWS)
            leaving[to, pair] = jnp.concatenate([whole[0, rows], whole[1, rows]], axis=0).astype(BF16)
        for step in range(1, X):
            leave(pair, step).start()
        final[x, pair] = leaving[x, pair]

    def write(pair):
        for step in range(1, X):
            leave(pair, step).wait_recv()
        for place in range(X):
            total = final[place, pair]
            at = place * (D // X) + pair * 2 * TILE
            sums[0, :, at : at + TILE] = total[:ROWS]
            sums[0, :, at + TILE : at + 2 * TILE] = total[ROWS:]

    late = {}
    late_tiles = {}
    for link in ("x+", "x-"):
        for i in range(Z):
            late[link, 0, "P", i] = ((), BAND * WIDTH * 2)
            late[link, 0, "Q", i] = (((link, 0, "P", i),), BAND * WIDTH)
        for tile in range(TILES // 2, TILES):
            key = (link, tile // 2 - 1, "W", tile)
            late[key] = ((), WIDTH * TILE * 2)
            late_tiles.setdefault(tile, []).append(key)
        for i in range(EARLY_FAR, TILES // 2):
            tile = FAR_TILES[link][i]
            key = (link, tile // 2 - 1, "U", i)
            late[key] = ((), WIDTH * TILE * 2)
            late_tiles.setdefault(tile, []).append(key)
    for way, link in ((1, "z+"), (-1, "z-")):
        for tile in range(TILES):
            rank = max(tile // 2 - 1, 0)
            for step in range(4):
                if step == 0 and starts_here(way, 1, tile):
                    continue
                away = way * (4 - step) if step else 4
                wanted = [(l, 0, "Q", n) for l in ("x+", "x-") for n, a in enumerate(NEAREST_LAST) if abs(a) == abs(away)]
                wanted += late_tiles.get(tile, [])
                if not starts_here(way, step, tile):
                    wanted.append((link, rank, "S", tile, step - 1))
                late[link, rank, "S", tile, step] = (tuple(wanted), BAND * TILE * 2)
    start, arrival = in_order(late, lambda key: 0.0)
    here = set()

    def need_late(key):
        if key not in here:
            here.add(key)
            link, kind, i = key
            if kind in "PQ":
                hand_context(link, 0 if kind == "P" else 1, i).wait_recv()
            else:
                need((link, 1, kind, i))

    events = [(t, 0, "copy", key) for key, t in start.items()]
    for pair in range(PAIRS):
        tiles = (2 * pair, 2 * pair + 1)
        there = max(arrival[link, max(pair - 1, 0), "S", tile, 3] for link in ("z+", "z-") for tile in tiles)
        events += [(there + 0.5, 1, "finish", pair), (there + 6.5, 2, "write", pair)]
    events.sort(key=lambda event: event[:2])
    for _, _, what, which in events:
        if what == "finish":
            finish(which)
        elif what == "write":
            write(which)
        elif which[2] == "P":
            hand_context(which[0], 0, which[3]).start()
        elif which[2] == "Q":
            need_late((which[0], "P", which[3]))
            hand_context(which[0], 1, which[3]).start()
        elif which[2] in "WU":
            if which[2] == "U":
                need((which[0], 1, "V", which[3]))
            weights((which[0], 1, which[2], which[3])).start()
        else:
            link, _, _, tile, step = which
            way = 1 if link == "z+" else -1
            make_terms(NEAREST_LAST.index(way * (4 - step) if step else 4), tile)
            hand_on(way, step, tile)

    for link in ("x+", "x-"):
        for i in range(TILES):
            weights((link, 1, "W", i)).wait_send()
        for i in range(TILES // 2):
            weights((link, 1, "V", i)).wait_send()
            weights((link, 1, "U", i)).wait_send()
        for i in range(Z):
            for hop in range(2):
                hand_context(link, hop, i).wait_send()
    for way in (1, -1):
        for tile in range(TILES):
            for step in range(4):
                if step or tile % 2 == (0 if way == 1 else 1):
                    handed(way, step, tile).wait_send()
    for pair in range(PAIRS):
        for step in range(1, X):
            leave(pair, step).wait_send()


def finish_kernel(summed, entering, attended, stream):
    attended[...] = summed[...]
    stream[...] = (entering[...].astype(F32) + summed[...].astype(F32)).astype(BF16)


def layer(arriving, norm_gain, w_query, w_key, w_value, w_out):
    any_space = pl.BlockSpec(memory_space=pl.ANY)
    vmem = pl.BlockSpec(memory_space=pltpu.VMEM)
    out = jax.ShapeDtypeStruct((1, ROWS, D), BF16)
    dma = pltpu.SemaphoreType.DMA
    summed, residual = pl.pallas_call(
        kernel,
        out_shape=(out, out),
        in_specs=[any_space, any_space, any_space, any_space, any_space, any_space],
        out_specs=(vmem, vmem),
        scratch_shapes=[
            pltpu.VMEM((1, LENGTH, WIDTH), BF16),
            pltpu.VMEM((1, D), BF16),
            pltpu.VMEM((N, LENGTH, WIDTH), BF16),
            pltpu.VMEM((WIDTH, D), BF16),
            pltpu.VMEM((2, 32, D), BF16),
            pltpu.VMEM((128, D), BF16),
            pltpu.VMEM((TILES, X * WIDTH, TILE), BF16),
            pltpu.VMEM((2, TILES // 2, WIDTH, TILE), BF16),
            pltpu.VMEM((LENGTH, WIDTH + 128), F32),
            pltpu.VMEM((LENGTH, 128), F32),
            pltpu.VMEM((LENGTH, HD), F32),
            pltpu.VMEM((LENGTH, HD), F32),
            pltpu.VMEM((LENGTH, HD), F32),
            pltpu.VMEM((LENGTH, WIDTH), BF16),
            pltpu.VMEM((KV_HEADS, 3, 16, 128), BF16),
            pltpu.VMEM((X, 2, 3, 16, 128), BF16),
            pltpu.VMEM((X, Z, 3, 16, 128), BF16),
            pltpu.VMEM((HD, LENGTH), BF16),
            pltpu.VMEM((HD, LENGTH), BF16),
            pltpu.VMEM((Z, BAND, WIDTH), F32),
            pltpu.VMEM((X, Z, BAND, WIDTH), BF16),
            pltpu.VMEM((Z, TILES, BAND, TILE), BF16),
            pltpu.VMEM((2, 4, TILES, BAND, TILE), BF16),
            pltpu.VMEM((2, BAND, TILE), F32),
            pltpu.VMEM((X, PAIRS, 2 * ROWS, TILE), BF16),
            pltpu.VMEM((X, PAIRS, 2 * ROWS, TILE), BF16),
            dma((2,)),
            dma((3,)),
            dma((TILES,)),
            dma((2,)),
            dma((2,)),
            dma((len(KEYS),)),
            dma((len(KEYS),)),
            dma((2, 2 * TILES)),
            dma((2, 2 * TILES)),
            dma((3, X - 1)),
            dma((3, X - 1)),
            dma((3, Z - 1)),
            dma((3, Z - 1)),
            dma((2, 2, Z)),
            dma((2, 2, Z)),
            dma((2, 4, TILES)),
            dma((2, 4, TILES)),
            dma((X - 1, PAIRS)),
            dma((X - 1, PAIRS)),
        ],
        compiler_params=pltpu.CompilerParams(
            collective_id=0, has_side_effects=True, vmem_limit_bytes=67043328
        ),
    )(arriving, norm_gain, w_query, w_key, w_value, w_out)
    return pl.pallas_call(finish_kernel, out_shape=(out, out), in_specs=[vmem, vmem], out_specs=(vmem, vmem))(summed, residual)


def solution(mesh):
    return jax.shard_map(
        layer,
        mesh=mesh,
        in_specs=(
            P("section", None, "mp"),
            P("section", None),
            P("section", "mp", None),
            P("section", "mp", None),
            P("section", "mp", None),
            P("section", "mp", None),
        ),
        out_specs=(P("section", "mp", None), P("section", "mp", None)),
        check_vma=False,
    )
```
